128 devices in a mesh: member: 8 (over x, core), region: 16 (over z, y).
Axes of the slice: x: 4, y: 4, z: 4, core: 2. Of those that a mesh axis runs over, the one named last changes fastest.
Arguments:
- ensemble: float32 [24, 32, 128, 512], P('member', 'region'), may hold values from -6 to 6
- obs_value: float32 [32, 128, 128], P(None, ('member', 'region')), may hold values from -6 to 6
- obs_error: float32 [32, 128, 128], P(None, ('member', 'region')), may hold values from 0.5 to 4
- obs_index: int32 [32, 128, 128], P(None, ('member', 'region')), may hold values from 0 to 511
- obs_count: int32 [32, 128], P(None, ('member', 'region')), may hold values from 1 to 128
Outputs:
- analysis: float32 [24, 32, 128, 512], P('member', 'region')
The draws below stay inside these ranges and needn't reach their ends.
Inputs may be any that keep to these rules, and one draw needn't show every extreme that they name: `obs_index`: value v names field v // (256) (0 SST, 1 SSH) at cell v mod (256) of the block, cells row-major. `obs_count`: slots below a block's count are observations; the others are padding and carry no weight.
All inputs are finite; a program needn't handle non-finite values.
Results may differ from the reference program's by a relative error of at most 0.0001.
Values sent between devices are 32-bit elements; how exact they have to be, the bound alone decides.
No kernel may reach another device: no remote copies, remote signals or barrier semaphores. Data moves between devices by JAX's collectives and lax.ppermute only.
A program may use at most 64 MiB of HBM per device.

```python
import math
import jax
import jax.numpy as jnp
from jax import lax

SIDE = 16
OBS = 128
NS_ITERS = 6
VALS = 512
MEMBERS = 24
BROWS = 32
BCOLS = 128


def set_ends(values, own_key, low, high):
    shape = values.shape
    place = [jax.random.randint(jax.random.fold_in(own_key, axis), (), 0, shape[axis]) for axis in range(len(shape))]
    values = values.at[tuple(place)].set(low)
    longest = shape.index(max(shape))
    place[longest] = (place[longest] + 1) % shape[longest]
    return values.at[tuple(place)].set(high)


def steps_of(key, extent, cuts, smallest, top_value):
    def one(dim, shards_of):
        draws = jax.random.uniform(jax.random.fold_in(jax.random.fold_in(key, 6), dim), (shards_of,), jnp.float32, smallest / len(cuts), top_value / len(cuts))
        return jnp.repeat(jnp.exp(draws), extent[dim] // shards_of).reshape((-1,) + (1,) * (len(extent) - dim - 1))

    loudness = one(*cuts[0])
    for cut in cuts[1:]:
        loudness = loudness * one(*cut)
    return loudness


def normal_values(key, shape, width, bound, shards=(), kind=jnp.bfloat16):
    result = jax.random.normal(key, shape, jnp.float32) * width
    if len(shards) > 0:
        result = steps_of(key, shape, shards, -0.22, 0.18) * result
    return jnp.clip(result, min=-bound, max=bound).astype(kind)


def setup_inputs(seed: int = 0) -> dict:
    streams_of = jax.random.split(jax.random.key(seed), 6)
    ensemble = normal_values(streams_of[0], (MEMBERS, BROWS, BCOLS, VALS), 1.0, 6.0, ((0, 8), (1, 16)), jnp.float32)
    obs_value = normal_values(streams_of[1], (BROWS, BCOLS, OBS), 1.0, 6.0, ((1, 128),), jnp.float32)
    obs_error = jnp.clip(jnp.exp(math.log(4.0) - 2.0794415 * jax.random.uniform(streams_of[2], (BROWS, BCOLS, OBS), jnp.float32) ** steps_of(streams_of[2], (BROWS, BCOLS, OBS), ((1, 128),), -0.2, 0.2)), 0.5, 4.0)
    obs_index = set_ends(jax.random.randint(streams_of[3], (BROWS, BCOLS, OBS), 0, VALS), jax.random.fold_in(streams_of[3], 1), 0, VALS - 1).astype(jnp.int32)
    obs_count = set_ends(jax.random.randint(streams_of[4], (BROWS, BCOLS), 1, OBS + 1), jax.random.fold_in(streams_of[4], 1), 1, OBS).astype(jnp.int32)
    return dict(ensemble=ensemble, obs_value=obs_value, obs_error=obs_error, obs_index=obs_index, obs_count=obs_count)


LOC_SCALE = 12.0
INFLATION_FACTOR = 1.1

def batch_product(left, right):
    return jnp.einsum('...ij,...jk->...ik', left, right, precision=lax.Precision.HIGHEST)

def observe(ensemble, obs_value, obs_error, obs_index, obs_count):
    ens_mean = lax.optimization_barrier(jnp.mean(ensemble, axis=0))
    anomaly = ensemble - ens_mean
    slot_index = lax.broadcasted_iota(jnp.int32, obs_index.shape, 2)
    live_slot = jnp.where(slot_index < obs_count[:, :, None], 1.0, 0.0).astype(jnp.float32)
    root_weight = jnp.sqrt(live_slot / obs_error)
    full_index = jnp.broadcast_to(obs_index[None], (anomaly.shape[0],) + obs_index.shape).astype(jnp.int32)
    seen_anom = jnp.take_along_axis(anomaly, full_index, axis=3)
    seen_mean = jnp.take_along_axis(ens_mean, obs_index.astype(jnp.int32), axis=2)
    rescaled_values = root_weight[:, :, None] * jnp.moveaxis(seen_anom, 0, 2)
    innovation = root_weight * (obs_value - seen_mean)
    cell_index = obs_index % (SIDE * SIDE)
    rowpos = (cell_index // SIDE).astype(jnp.float32)
    column_position = (cell_index % SIDE).astype(jnp.float32)
    stacked = jnp.concatenate([rescaled_values, innovation[:, :, None], rowpos[:, :, None], column_position[:, :, None]], axis=2)
    return (anomaly, ens_mean, stacked)

def analyze(anomaly, ens_mean, padded):
    ensemble_members = anomaly.shape[0]
    row_count = anomaly.shape[1]
    col_count = anomaly.shape[2]
    pieces = []
    for row_step in range(3):
        for col_step in range(3):
            pieces.append(padded[row_step:row_step + row_count, col_step:col_step + col_count])
    nearby = jnp.stack(pieces, axis=2)
    rescaled_values = nearby[:, :, :, :ensemble_members]
    innovation = nearby[:, :, :, ensemble_members]
    rowpos = nearby[:, :, :, ensemble_members + 1]
    column_position = nearby[:, :, :, ensemble_members + 2]
    offset_index = jnp.arange(9, dtype=jnp.int32)
    offset_row = (offset_index // 3 - 1).astype(jnp.float32) * SIDE
    offset_col = (offset_index % 3 - 1).astype(jnp.float32) * SIDE
    half_side = SIDE // 2
    point_index = jnp.arange(4, dtype=jnp.int32)
    center_row = (point_index // 2).astype(jnp.float32) * half_side + (half_side - 1) * 0.5
    center_col = (point_index % 2).astype(jnp.float32) * half_side + (half_side - 1) * 0.5
    row_gap = offset_row[:, None] + rowpos
    col_gap = offset_col[:, None] + column_position
    distance = (row_gap[:, :, None] - center_row[:, None, None]) ** 2 + (col_gap[:, :, None] - center_col[:, None, None]) ** 2
    locality = jnp.exp(-distance / (2.0 * LOC_SCALE * LOC_SCALE))
    weighted = locality[:, :, :, :, None, :] * rescaled_values[:, :, None]
    gramian_total = jnp.einsum('rcpnko,rcnjo->rcpkj', weighted, rescaled_values, precision=lax.Precision.HIGHEST)
    drive_vec = jnp.einsum('rcpnko,rcno->rcpk', weighted, innovation, precision=lax.Precision.HIGHEST)
    identity_matrix = jnp.eye(ensemble_members, dtype=jnp.float32)
    precision_matrix = gramian_total + (ensemble_members - 1) / INFLATION_FACTOR * identity_matrix
    norm_scale = jnp.sqrt(lax.optimization_barrier(jnp.sum(precision_matrix * precision_matrix, axis=(3, 4), keepdims=True)))
    root_iter = precision_matrix / norm_scale
    inv_iter = jnp.broadcast_to(identity_matrix, precision_matrix.shape)
    for sweep_index in range(NS_ITERS):
        ns_step = 1.5 * identity_matrix - 0.5 * batch_product(inv_iter, root_iter)
        root_iter = batch_product(root_iter, ns_step)
        inv_iter = batch_product(ns_step, inv_iter)
    inv_root = inv_iter / jnp.sqrt(norm_scale)
    half_way = jnp.einsum('rcpkj,rcpj->rcpk', inv_root, drive_vec, precision=lax.Precision.HIGHEST)
    mean_w = jnp.einsum('rcpkj,rcpj->rcpk', inv_root, half_way, precision=lax.Precision.HIGHEST)
    weights = mean_w[..., :, None] + math.sqrt(ensemble_members - 1) * inv_root
    point_weights = weights.reshape(row_count, col_count, 2, 2, ensemble_members, ensemble_members)
    shaped = anomaly.reshape(ensemble_members, row_count, col_count, 2, 2, half_side, 2, half_side)
    updated = jnp.einsum('jrcvaybx,rcabjk->krcvaybx', shaped, point_weights, precision=lax.Precision.HIGHEST)
    return ens_mean[None] + updated.reshape(anomaly.shape)

def reference(ensemble, obs_value, obs_error, obs_index, obs_count):
    anomaly, ens_mean, stacked = observe(ensemble, obs_value, obs_error, obs_index, obs_count)
    padded = jnp.pad(stacked, ((1, 1), (1, 1), (0, 0), (0, 0)))

    def one_row(row_index):
        part_anom = lax.dynamic_slice_in_dim(anomaly, row_index, 1, 1)
        part_mean = lax.dynamic_slice_in_dim(ens_mean, row_index, 1, 0)
        part_pad = lax.dynamic_slice_in_dim(padded, row_index, 3, 0)
        return analyze(part_anom, part_mean, part_pad)
    row_results = lax.map(one_row, jnp.arange(BROWS, dtype=jnp.int32))
    return jnp.moveaxis(row_results[:, :, 0], 0, 1)
```

```python
import math

import jax
import jax.numpy as jnp
from jax import lax
from jax.experimental import pallas as pl
from jax.experimental.pallas import tpu as pltpu
from jax.sharding import PartitionSpec as P

SIDE = 16
NS_ITERS = 6
MEMBERS = 24
OBS = 128
VALS = 512
INFLATION_FACTOR = 1.1
INV_SCALE = 1.0 / 288.0

ROWS = 2
COLS = 16
BLOCKS = ROWS * COLS
POINTS = 4
EXT_COLS = COLS + 2
EXT = (ROWS + 2) * EXT_COLS
SLAB = 32
STRIDE = BLOCKS * 4


def observe_kernel(ens_ref, obs_ref, out_ref):
    sub = lax.broadcasted_iota(jnp.int32, (8, OBS), 0)

    def body(c, carry):
        obs = obs_ref[c]
        for i in range(ROWS):
            value = obs[i : i + 1]
            weight = obs[2 + i : 3 + i]
            index_f = obs[4 + i : 5 + i]
            index = jnp.broadcast_to(index_f.astype(jnp.int32), (MEMBERS, OBS))
            lane = index & 127
            chunk = index >> 7
            first = (2 * i + (c >> 3)) * 32 + (c & 7)
            seen = jnp.zeros((MEMBERS, OBS), jnp.float32)
            for t in range(4):
                ens = ens_ref[pl.ds(first + 8 * t, MEMBERS, stride=STRIDE), :]
                got = jnp.take_along_axis(ens, lane, axis=1, mode="promise_in_bounds")
                seen = jnp.where(chunk == t, got, seen)
            mean = jnp.sum(seen, axis=0, keepdims=True) * (1.0 / MEMBERS)
            out_ref[i, c, 0:MEMBERS, :] = weight * (seen - mean)
            innovation = weight * (value - mean)
            out_ref[i, c, MEMBERS:SLAB, :] = jnp.where(
                sub == 0, innovation, jnp.where(sub == 1, index_f, 0.0)
            )
        return carry

    lax.fori_loop(0, COLS, body, 0)


def split_bf16(x):
    high = x.astype(jnp.bfloat16)
    low = (x - high.astype(jnp.float32)).astype(jnp.bfloat16)
    return high, low


def sym_product(left, right, out, finish):
    for tile in range(3):
        lo = 8 * tile
        for half in range(2):
            i0 = lo + 4 * half
            acc = None
            for k in range(MEMBERS):
                term = left[i0 : i0 + 4, k : k + 1, :] * right[k : k + 1, lo:MEMBERS, :]
                acc = term if acc is None else acc + term
            for step in range(4):
                i = i0 + step
                row = finish(acc[step], i, lo)
                out[i, lo:MEMBERS, :] = row
                for j in range(tile + 1, 3):
                    out[8 * j : 8 * j + 8, i, :] = row[8 * (j - tile) : 8 * (j - tile) + 8]


def plain(row, i, lo):
    return row


def newton_step(row, i, lo):
    where = lax.broadcasted_iota(jnp.int32, row.shape, 0) + lo
    return jnp.where(where == i, 1.5, 0.0) - 0.5 * row


def analyze_kernel(
    ens_ref, own_ref, top_ref, bot_ref, left_ref, right_ref, out_ref,
    source, pair, locs, gram, ya, yb, za, zb, mm, drive,
):
    t = lax.broadcasted_iota(jnp.int32, (8, OBS), 0)
    offset = (((t >> 1) - 1) * SIDE - (t & 1) * 8).astype(jnp.float32) - 3.5

    def put(slot, slab):
        cell = slab[25:26].astype(jnp.int32) & 255
        dy = (cell >> 4).astype(jnp.float32) + offset
        dx = (cell & 15).astype(jnp.float32) + offset
        locs[slot, 0:8, :] = jnp.exp(-(dy * dy) * INV_SCALE)
        locs[slot, 8:16, :] = jnp.exp(-(dx * dx) * INV_SCALE)
        source[slot] = slab[0:MEMBERS]
        high, low = split_bf16(slab)
        pair[slot] = jnp.concatenate([high, low], axis=0)

    def put_column(c, carry):
        for i in range(ROWS):
            put((i + 1) * EXT_COLS + 1 + c, own_ref[i, c])
        return carry

    def put_edge(c, carry):
        put(c, top_ref[c])
        put((ROWS + 1) * EXT_COLS + c, bot_ref[c])
        return carry

    lax.fori_loop(0, COLS, put_column, 0)
    lax.fori_loop(0, EXT_COLS, put_edge, 0)
    for i in range(ROWS):
        put((i + 1) * EXT_COLS, left_ref[i, 0])
        put((i + 1) * EXT_COLS + EXT_COLS - 1, right_ref[i, 0])

    def one_gram(c, carry):
        for i in range(ROWS):
            acc = jnp.zeros((POINTS * MEMBERS, 2 * SLAB), jnp.float32)
            for di in range(3):
                for dj in range(3):
                    slot = (i + di) * EXT_COLS + c + dj
                    loc = locs[slot]
                    base = source[slot]
                    rows = []
                    for a in range(2):
                        for b in range(2):
                            w = loc[2 * di + a : 2 * di + a + 1] * loc[8 + 2 * dj + b : 9 + 2 * dj + b]
                            rows.append(w * base)
                    high, low = split_bf16(jnp.concatenate(rows, axis=0))
                    both = pair[slot]
                    acc = acc + lax.dot_general(
                        jnp.concatenate([high, low], axis=1),
                        jnp.concatenate([both, both], axis=1),
                        (((1,), (1,)), ((), ())),
                        preferred_element_type=jnp.float32,
                    )
            start = pl.multiple_of((i * COLS + c) * (POINTS * MEMBERS), 8)
            gram[pl.ds(start, POINTS * MEMBERS), 0 : 2 * SLAB] = acc
        return carry

    lax.fori_loop(0, COLS, one_gram, 0)

    member = lax.broadcasted_iota(jnp.int32, (MEMBERS, 128), 0)
    squares = jnp.zeros((MEMBERS, 128), jnp.float32)
    for k in range(MEMBERS):
        turned = gram[pl.ds(k, 128, stride=MEMBERS), :].T
        total = turned[0:SLAB] + turned[SLAB : 2 * SLAB]
        row = total[0:MEMBERS] + jnp.where(member == k, (MEMBERS - 1) / INFLATION_FACTOR, 0.0)
        drive[k : k + 1, :] = total[MEMBERS : MEMBERS + 1]
        ya[k] = row
        squares = squares + row * row
    norm = jnp.sqrt(jnp.sum(squares, axis=0, keepdims=True))
    inverse = 1.0 / norm
    for k in range(MEMBERS):
        row = ya[k] * inverse
        ya[k] = row
        za[k] = newton_step(row, k, 0)

    sym_product(ya, za, yb, plain)

    def two_steps(turn, carry):
        sym_product(za, yb, mm, newton_step)
        sym_product(yb, mm, ya, plain)
        sym_product(mm, za, zb, plain)
        sym_product(zb, ya, mm, newton_step)
        sym_product(ya, mm, yb, plain)
        sym_product(mm, zb, za, plain)
        return carry

    lax.fori_loop(0, (NS_ITERS - 2) // 2, two_steps, 0)
    sym_product(za, yb, mm, newton_step)
    sym_product(mm, za, zb, plain)

    scale = 1.0 / jnp.sqrt(norm)
    half_way = jnp.zeros((MEMBERS, 128), jnp.float32)
    for k in range(MEMBERS):
        half_way = half_way + zb[k] * drive[k : k + 1, :]
    half_way = half_way * scale
    mean_w = jnp.zeros((MEMBERS, 128), jnp.float32)
    for k in range(MEMBERS):
        mean_w = mean_w + zb[k] * half_way[k : k + 1]
    mean_w = mean_w * scale
    spread = scale * math.sqrt(MEMBERS - 1)
    blank = jnp.zeros((128 - 3 * MEMBERS, 128), jnp.float32)
    for k in range(MEMBERS):
        weight = mean_w + spread * zb[k]
        high = weight.astype(jnp.bfloat16).astype(jnp.float32)
        gram[pl.ds(k, 128, stride=MEMBERS), :] = jnp.concatenate(
            [high, high, weight - high, blank], axis=0
        ).T

    right_half = (lax.broadcasted_iota(jnp.int32, (MEMBERS, 128), 1) >> 3) & 1

    def one_update(c, carry):
        for i in range(ROWS):
            block = i * COLS + c
            start = pl.multiple_of(block * (POINTS * MEMBERS), 8)
            weight = gram[pl.ds(start, POINTS * MEMBERS), :].astype(jnp.bfloat16)
            first = (2 * i + (c >> 3)) * 32 + (c & 7)
            ens = jnp.concatenate(
                [ens_ref[pl.ds(first + 8 * t, MEMBERS, stride=STRIDE), :] for t in range(4)], axis=1
            )
            mean = jnp.sum(ens, axis=0, keepdims=True) * (1.0 / MEMBERS)
            anomaly = ens - mean
            high = anomaly.astype(jnp.bfloat16).astype(jnp.float32)
            low = anomaly - high
            stacked = jnp.concatenate(
                [high, low, high, jnp.zeros((128 - 3 * MEMBERS, VALS), jnp.float32)], axis=0
            ).astype(jnp.bfloat16)
            for a in range(2):
                values = jnp.concatenate(
                    [stacked[:, 128 * a : 128 * a + 128], stacked[:, 256 + 128 * a : 384 + 128 * a]], axis=1
                )
                moved = jnp.dot(
                    weight[48 * a : 48 * a + 48], values, preferred_element_type=jnp.float32
                )
                for f in range(2):
                    part = moved[:, 128 * f : 128 * f + 128]
                    t = 2 * f + a
                    moved_tile = jnp.where(right_half == 1, part[MEMBERS:], part[:MEMBERS])
                    out_ref[pl.ds(first + 8 * t, MEMBERS, stride=STRIDE), :] = (
                        mean[:, 128 * t : 128 * t + 128] + moved_tile
                    )
        return carry

    lax.fori_loop(0, COLS, one_update, 0)


def vmem_call(kernel, shape, scratch=()):
    return pl.pallas_call(
        kernel,
        out_shape=jax.ShapeDtypeStruct(shape, jnp.float32),
        scratch_shapes=list(scratch),
        compiler_params=pltpu.CompilerParams(vmem_limit_bytes=40 * 1024 * 1024),
    )


def shifted(x, axis, by):
    devices = lax.axis_size(axis)
    pairs = [(i, i + by) for i in range(devices) if 0 <= i + by < devices]
    return lax.ppermute(x, axis, pairs)


def local(ensemble, obs_value, obs_error, obs_index, obs_count):
    tiled = ensemble.reshape(3, ROWS, 8, 2, 8, 4, 128).transpose(2, 0, 1, 3, 5, 4, 6)
    by_block = lax.all_to_all(tiled, "member", split_axis=0, concat_axis=0, tiled=True)
    by_block = by_block.reshape(MEMBERS * STRIDE, 128)

    slot = lax.broadcasted_iota(jnp.int32, (32, 1, OBS), 2)
    live = jnp.where(slot < obs_count[:, :, None], 1.0, 0.0).astype(jnp.float32)
    root_weight = jnp.sqrt(live / obs_error)
    pieces = [obs_value, root_weight, obs_index.astype(jnp.float32), jnp.zeros_like(obs_value)]
    packed = jnp.concatenate([x.reshape(COLS, ROWS, OBS) for x in pieces], axis=1)
    obs = lax.all_to_all(packed, "region", split_axis=0, concat_axis=0, tiled=True)

    own = vmem_call(observe_kernel, (ROWS, COLS, SLAB, OBS))(by_block, obs)

    left = shifted(own[:, COLS - 1 :], "member", 1)
    right = shifted(own[:, :1], "member", -1)
    top = shifted(jnp.concatenate([left[1], own[1], right[1]], axis=0), "region", 1)
    bot = shifted(jnp.concatenate([left[0], own[0], right[0]], axis=0), "region", -1)

    square = pltpu.VMEM((MEMBERS, MEMBERS, 128), jnp.float32)
    result = vmem_call(
        analyze_kernel,
        (MEMBERS * STRIDE, 128),
        (
            pltpu.VMEM((EXT, MEMBERS, OBS), jnp.float32),
            pltpu.VMEM((EXT, 2 * SLAB, OBS), jnp.bfloat16),
            pltpu.VMEM((EXT, 16, OBS), jnp.float32),
            pltpu.VMEM((BLOCKS * POINTS * MEMBERS, 128), jnp.float32),
            square, square, square, square, square,
            pltpu.VMEM((MEMBERS, 128), jnp.float32),
        ),
    )(by_block, own, top, bot, left, right)
    result = result.reshape(8, 3, ROWS, 2, 4, 8, 128)
    by_member = lax.all_to_all(result, "member", split_axis=0, concat_axis=0, tiled=True)
    return by_member.transpose(1, 2, 0, 3, 5, 4, 6).reshape(3, ROWS, 8 * COLS, VALS)


def solution(mesh):
    return jax.shard_map(
        local,
        mesh=mesh,
        in_specs=(
            P("member", "region", None, None),
            P(None, ("member", "region"), None),
            P(None, ("member", "region"), None),
            P(None, ("member", "region"), None),
            P(None, ("member", "region")),
        ),
        out_specs=P("member", "region", None, None),
        check_vma=False,
    )
```

```python
import math

import jax
import jax.numpy as jnp
from jax import lax
from jax.experimental import pallas as pl
from jax.experimental.pallas import tpu as pltpu
from jax.sharding import PartitionSpec as P


SIDE = 16
NS_ITERS = 6
MEMBERS = 24
OBS = 128
VALS = 512
INFLATION_FACTOR = 1.1
INV_SCALE = 1.0 / 288.0

GROUPS = 8
HELD = MEMBERS // GROUPS
ROWS = 2
COLS = 16
BLOCKS = ROWS * COLS
POINTS = 4
EXT_COLS = COLS + 2
FIELD_ROWS = BLOCKS * 4
PITCH = FIELD_ROWS + 4
SLAB = 26
WIDE = 32
MAT = MEMBERS + 4
BLOCK_MAT = POINTS * MAT


def first_row(i, c):
    return i * 64 + (c >> 3) * 32 + (c & 7)


def split_bf16(x):
    high = x.astype(jnp.bfloat16)
    low = (x - high.astype(jnp.float32)).astype(jnp.bfloat16)
    return high, low


def observe_kernel(m_ref, *refs):
    parts = refs[:GROUPS]
    obs_ref, ens_ref, slab_ref, left_ref, right_ref = refs[GROUPS:]
    m = m_ref[0]
    for s in range(GROUPS):
        for k in range(HELD):
            start = ((m ^ s) * HELD + k) * PITCH
            ens_ref[pl.ds(start, FIELD_ROWS), :] = parts[s][k * FIELD_ROWS : (k + 1) * FIELD_ROWS, :]

    def body(c, carry):
        obs = obs_ref[c]
        for i in range(ROWS):
            value = obs[i : i + 1]
            weight = obs[2 + i : 3 + i]
            index_f = obs[4 + i : 5 + i]
            index = jnp.broadcast_to(index_f.astype(jnp.int32), (MEMBERS, OBS))
            lane = index & 127
            chunk = index >> 7
            seen = jnp.zeros((MEMBERS, OBS), jnp.float32)
            for t in range(4):
                ens = ens_ref[pl.ds(first_row(i, c) + 8 * t, MEMBERS, stride=PITCH), :]
                got = jnp.take_along_axis(ens, lane, axis=1, mode="promise_in_bounds")
                seen = jnp.where(chunk == t, got, seen)
            mean = jnp.sum(seen, axis=0, keepdims=True) * (1.0 / MEMBERS)
            base = (i * COLS + c) * SLAB
            slab_ref[pl.ds(base, MEMBERS), :] = weight * (seen - mean)
            slab_ref[pl.ds(base + MEMBERS, 1), :] = weight * (value - mean)
            slab_ref[pl.ds(base + MEMBERS + 1, 1), :] = index_f
        return carry

    lax.fori_loop(0, COLS, body, 0)
    for i in range(ROWS):
        west = i * COLS * SLAB
        east = west + (COLS - 1) * SLAB
        left_ref[i * WIDE : i * WIDE + SLAB, :] = slab_ref[west : west + SLAB, :]
        right_ref[i * WIDE : i * WIDE + SLAB, :] = slab_ref[east : east + SLAB, :]


def put_slab(slot, ref, base, source, pair, locs):
    t = lax.broadcasted_iota(jnp.int32, (8, OBS), 0)
    offset = (((t >> 1) - 1) * SIDE - (t & 1) * 8).astype(jnp.float32) - 3.5
    cell = ref[pl.ds(base + MEMBERS + 1, 1), :].astype(jnp.int32) & 255
    dy = (cell >> 4).astype(jnp.float32) + offset
    dx = (cell & 15).astype(jnp.float32) + offset
    locs[slot, 0:8, :] = jnp.exp(-(dy * dy) * INV_SCALE)
    locs[slot, 8:16, :] = jnp.exp(-(dx * dx) * INV_SCALE)
    scaled = ref[pl.ds(base, MEMBERS), :]
    source[slot] = scaled
    innovation = jnp.broadcast_to(ref[pl.ds(base + MEMBERS, 1), :], (8, OBS))
    high, low = split_bf16(jnp.concatenate([scaled, innovation], axis=0))
    pair[slot] = jnp.concatenate([high, low], axis=0)


def contribution(slot, di, dj, source, pair, locs):
    loc = locs[slot]
    base = source[slot]
    rows = []
    for a in range(2):
        for b in range(2):
            w = loc[2 * di + a : 2 * di + a + 1] * loc[8 + 2 * dj + b : 9 + 2 * dj + b]
            rows.append(w * base)
    high, low = split_bf16(jnp.concatenate(rows, axis=0))
    both = pair[slot]
    return lax.dot_general(
        jnp.concatenate([high, low], axis=1),
        jnp.concatenate([both, both], axis=1),
        (((1,), (1,)), ((), ())),
        preferred_element_type=jnp.float32,
    )


def own_gram_kernel(slab_ref, gram_ref, source, pair, locs):
    for i in range(ROWS):
        for c in (0, EXT_COLS - 1):
            source[i * EXT_COLS + c] = jnp.zeros((MEMBERS, OBS), jnp.float32)
            pair[i * EXT_COLS + c] = jnp.zeros((2 * WIDE, OBS), jnp.bfloat16)
            locs[i * EXT_COLS + c] = jnp.zeros((16, OBS), jnp.float32)

    def put(c, carry):
        for i in range(ROWS):
            put_slab(i * EXT_COLS + c + 1, slab_ref, (i * COLS + c) * SLAB, source, pair, locs)
        return carry

    lax.fori_loop(0, COLS, put, 0)

    def one(c, carry):
        for i in range(ROWS):
            acc = jnp.zeros((POINTS * MEMBERS, 2 * WIDE), jnp.float32)
            for q in range(ROWS):
                for dj in range(3):
                    acc = acc + contribution(q * EXT_COLS + c + dj, q - i + 1, dj, source, pair, locs)
            for p in range(POINTS):
                gram_ref[pl.ds((i * COLS + c) * BLOCK_MAT + p * MAT, MEMBERS), 0 : 2 * WIDE] = acc[
                    p * MEMBERS : (p + 1) * MEMBERS
                ]
        return carry

    lax.fori_loop(0, COLS, one, 0)


def sym_product(left, right, out, finish):
    for tile in range(3):
        lo = 8 * tile
        for half in range(2):
            i0 = lo + 4 * half
            acc = [None] * 4
            for k in range(MEMBERS):
                row = right[k * MAT + lo : k * MAT + MEMBERS, :]
                for step in range(4):
                    at = (i0 + step) * MAT + k
                    term = left[at : at + 1, :] * row
                    acc[step] = term if acc[step] is None else acc[step] + term
            for step in range(4):
                i = i0 + step
                row = finish(acc[step], i, lo)
                out[i * MAT + lo : i * MAT + MEMBERS, :] = row
                for j in range(tile + 1, 3):
                    out[pl.ds(8 * j * MAT + i, 8, stride=MAT), :] = row[8 * (j - tile) : 8 * (j - tile) + 8]


def plain(row, i, lo):
    return row


def newton_step(row, i, lo):
    where = lax.broadcasted_iota(jnp.int32, row.shape, 0) + lo
    return jnp.where(where == i, 1.5, 0.0) - 0.5 * row


def analyze_kernel(m_ref, ens_ref, own_ref, above_ref, below_ref, left_ref, right_ref, *refs):
    corners = refs[:4]
    outs = refs[4 : 4 + GROUPS]
    source, pair, locs, gram, ya, yb, za, zb, mm, drive, moved_ref = refs[4 + GROUPS :]
    m = m_ref[0]

    def put(c, carry):
        put_slab(c + 1, above_ref, c * SLAB, source, pair, locs)
        put_slab(EXT_COLS + c + 1, below_ref, c * SLAB, source, pair, locs)
        return carry

    lax.fori_loop(0, COLS, put, 0)
    for n, slot in enumerate((0, EXT_COLS - 1, EXT_COLS, 2 * EXT_COLS - 1)):
        put_slab(slot, corners[n], 0, source, pair, locs)
    side = 2 * EXT_COLS
    for q in range(ROWS):
        put_slab(side + q, left_ref, q * WIDE, source, pair, locs)
        put_slab(side + ROWS + q, right_ref, q * WIDE, source, pair, locs)

    def one_gram(c, carry):
        for i in range(ROWS):
            acc = jnp.zeros((POINTS * MEMBERS, 2 * WIDE), jnp.float32)
            for dj in range(3):
                acc = acc + contribution(i * EXT_COLS + c + dj, 2 * i, dj, source, pair, locs)
            for p in range(POINTS):
                at = (i * COLS + c) * BLOCK_MAT + p * MAT
                gram[pl.ds(at, MEMBERS), 0 : 2 * WIDE] = (
                    own_ref[pl.ds(at, MEMBERS), 0 : 2 * WIDE] + acc[p * MEMBERS : (p + 1) * MEMBERS]
                )
        return carry

    lax.fori_loop(0, COLS, one_gram, 0)
    for i in range(ROWS):
        for edge in range(2):
            acc = jnp.zeros((POINTS * MEMBERS, 2 * WIDE), jnp.float32)
            for q in range(ROWS):
                acc = acc + contribution(side + ROWS * edge + q, q - i + 1, 2 * edge, source, pair, locs)
            for p in range(POINTS):
                at = (i * COLS + edge * (COLS - 1)) * BLOCK_MAT + p * MAT
                gram[at : at + MEMBERS, 0 : 2 * WIDE] = (
                    gram[at : at + MEMBERS, 0 : 2 * WIDE] + acc[p * MEMBERS : (p + 1) * MEMBERS]
                )

    member = lax.broadcasted_iota(jnp.int32, (MEMBERS, 128), 0)
    squares = jnp.zeros((MEMBERS, 128), jnp.float32)
    for k in range(MEMBERS):
        turned = gram[pl.ds(k, 128, stride=MAT), :].T
        total = turned[0:WIDE] + turned[WIDE : 2 * WIDE]
        row = total[0:MEMBERS] + jnp.where(member == k, (MEMBERS - 1) / INFLATION_FACTOR, 0.0)
        drive[k : k + 1, :] = total[MEMBERS : MEMBERS + 1]
        ya[k * MAT : k * MAT + MEMBERS, :] = row
        squares = squares + row * row
    norm = jnp.sqrt(jnp.sum(squares, axis=0, keepdims=True))
    inverse = 1.0 / norm
    for k in range(MEMBERS):
        row = ya[k * MAT : k * MAT + MEMBERS, :] * inverse
        ya[k * MAT : k * MAT + MEMBERS, :] = row
        za[k * MAT : k * MAT + MEMBERS, :] = newton_step(row, k, 0)

    sym_product(ya, za, yb, plain)

    def two_steps(turn, carry):
        sym_product(za, yb, mm, newton_step)
        sym_product(yb, mm, ya, plain)
        sym_product(mm, za, zb, plain)
        sym_product(zb, ya, mm, newton_step)
        sym_product(ya, mm, yb, plain)
        sym_product(mm, zb, za, plain)
        return carry

    lax.fori_loop(0, (NS_ITERS - 2) // 2, two_steps, 0)
    sym_product(za, yb, mm, newton_step)
    sym_product(mm, za, zb, plain)

    scale = 1.0 / jnp.sqrt(norm)
    half_way = jnp.zeros((MEMBERS, 128), jnp.float32)
    for k in range(MEMBERS):
        half_way = half_way + zb[k * MAT : k * MAT + MEMBERS, :] * drive[k : k + 1, :]
    half_way = half_way * scale
    mean_w = jnp.zeros((MEMBERS, 128), jnp.float32)
    for k in range(MEMBERS):
        mean_w = mean_w + zb[k * MAT : k * MAT + MEMBERS, :] * half_way[k : k + 1]
    mean_w = mean_w * scale
    spread = scale * math.sqrt(MEMBERS - 1)
    blank = jnp.zeros((128 - 3 * MEMBERS, 128), jnp.float32)
    for k in range(MEMBERS):
        weight = mean_w + spread * zb[k * MAT : k * MAT + MEMBERS, :]
        high = weight.astype(jnp.bfloat16).astype(jnp.float32)
        gram[pl.ds(k, 128, stride=MAT), :] = jnp.concatenate(
            [high, high, weight - high, blank], axis=0
        ).T

    right_half = (lax.broadcasted_iota(jnp.int32, (MEMBERS, 128), 1) >> 3) & 1

    def one_update(c, carry):
        for i in range(ROWS):
            at = (i * COLS + c) * BLOCK_MAT
            first = first_row(i, c)
            ens = jnp.concatenate(
                [ens_ref[pl.ds(first + 8 * t, MEMBERS, stride=PITCH), :] for t in range(4)], axis=1
            )
            mean = jnp.sum(ens, axis=0, keepdims=True) * (1.0 / MEMBERS)
            anomaly = ens - mean
            high = anomaly.astype(jnp.bfloat16).astype(jnp.float32)
            low = anomaly - high
            stacked = jnp.concatenate(
                [high, low, high, jnp.zeros((128 - 3 * MEMBERS, VALS), jnp.float32)], axis=0
            ).astype(jnp.bfloat16)
            for a in range(2):
                values = jnp.concatenate(
                    [stacked[:, 128 * a : 128 * a + 128], stacked[:, 256 + 128 * a : 384 + 128 * a]], axis=1
                )
                weight = jnp.concatenate(
                    [gram[pl.ds(at + (2 * a + b) * MAT, MEMBERS), :] for b in range(2)], axis=0
                ).astype(jnp.bfloat16)
                moved = jnp.dot(weight, values, preferred_element_type=jnp.float32)
                for f in range(2):
                    part = moved[:, 128 * f : 128 * f + 128]
                    t = 2 * f + a
                    moved_tile = jnp.where(right_half == 1, part[MEMBERS:], part[:MEMBERS])
                    moved_ref[pl.ds(first + 8 * t, MEMBERS, stride=PITCH), :] = (
                        mean[:, 128 * t : 128 * t + 128] + moved_tile
                    )
        return carry

    lax.fori_loop(0, COLS, one_update, 0)
    for s in range(GROUPS):
        for k in range(HELD):
            start = ((m ^ s) * HELD + k) * PITCH
            outs[s][k * FIELD_ROWS : (k + 1) * FIELD_ROWS, :] = moved_ref[pl.ds(start, FIELD_ROWS), :]


def f32(*shape):
    return jax.ShapeDtypeStruct(shape, jnp.float32)


def tables(slots):
    return [
        pltpu.VMEM((slots, MEMBERS, OBS), jnp.float32),
        pltpu.VMEM((slots, 2 * WIDE, OBS), jnp.bfloat16),
        pltpu.VMEM((slots, 16, OBS), jnp.float32),
    ]


def vmem_call(kernel, out_shape, flops, args, scratch=()):
    places = [
        pl.BlockSpec(memory_space=pltpu.SMEM if x.dtype == jnp.int32 else pltpu.VMEM) for x in args
    ]
    return pl.pallas_call(
        kernel,
        out_shape=out_shape,
        in_specs=places,
        scratch_shapes=list(scratch),
        cost_estimate=pl.CostEstimate(flops=flops, bytes_accessed=0, transcendentals=0),
        compiler_params=pltpu.CompilerParams(vmem_limit_bytes=32 * 1024 * 1024),
    )(*args)


def swapped(x, s):
    return lax.ppermute(x, "member", [(a, a ^ s) for a in range(GROUPS)])


def neighbour(x, dm, dr):
    members, regions = lax.axis_size("member"), lax.axis_size("region")
    pairs = []
    for a in range(members):
        for b in range(regions):
            if 0 <= a + dm < members and 0 <= b + dr < regions:
                pairs.append((a * regions + b, (a + dm) * regions + b + dr))
    return lax.ppermute(x, ("member", "region"), pairs)


def local(ensemble, obs_value, obs_error, obs_index, obs_count):
    m = lax.axis_index("member").astype(jnp.int32)
    where = m.reshape(1)
    tiled = ensemble.reshape(HELD, ROWS, GROUPS, 2, 8, 4, 128).transpose(2, 0, 1, 3, 5, 4, 6)
    parts = []
    for s in range(GROUPS):
        part = lax.dynamic_index_in_dim(tiled, m ^ s, 0, keepdims=False)
        part = part.reshape(HELD * FIELD_ROWS, 128)
        parts.append(swapped(part, s) if s else part)

    slot = lax.broadcasted_iota(jnp.int32, (32, 1, OBS), 2)
    live = jnp.where(slot < obs_count[:, :, None], 1.0, 0.0).astype(jnp.float32)
    root_weight = jnp.sqrt(live / obs_error)
    pieces = [obs_value, root_weight, obs_index.astype(jnp.float32), jnp.zeros_like(obs_value)]
    packed = jnp.concatenate([x.reshape(COLS, ROWS, OBS) for x in pieces], axis=1)
    obs = lax.all_to_all(packed, "region", split_axis=0, concat_axis=0, tiled=True)

    ens, slabs, west, east = vmem_call(
        observe_kernel,
        (
            f32(MEMBERS * PITCH, 128),
            f32(BLOCKS * SLAB, OBS),
            f32(ROWS * WIDE, OBS),
            f32(ROWS * WIDE, OBS),
        ),
        10**9,
        [where, *parts, obs],
    )

    half = COLS * SLAB
    below = neighbour(slabs[:half], 0, -1)
    above = neighbour(slabs[half:], 0, 1)
    right = neighbour(west, -1, 0)
    left = neighbour(east, 1, 0)
    corners = [
        neighbour(east[WIDE:], 1, 1),
        neighbour(west[WIDE:], -1, 1),
        neighbour(east[:WIDE], 1, -1),
        neighbour(west[:WIDE], -1, -1),
    ]

    own = vmem_call(
        own_gram_kernel,
        f32(BLOCKS * BLOCK_MAT, 128),
        4 * 10**9,
        [slabs],
        tables(ROWS * EXT_COLS),
    )

    square = pltpu.VMEM((MEMBERS * MAT, 128), jnp.float32)
    moved = vmem_call(
        analyze_kernel,
        [f32(HELD * FIELD_ROWS, 128)] * GROUPS,
        10**10,
        [where, ens, own, above, below, left, right, *corners],
        tables(ROWS * EXT_COLS + 2 * ROWS)
        + [
            pltpu.VMEM((BLOCKS * BLOCK_MAT, 128), jnp.float32),
            square, square, square, square, square,
            pltpu.VMEM((MEMBERS, 128), jnp.float32),
            pltpu.VMEM((MEMBERS * PITCH, 128), jnp.float32),
        ],
    )

    result = jnp.zeros((HELD, ROWS, GROUPS, 2, 4, 8, 128), jnp.float32)
    for s in range(GROUPS):
        part = swapped(moved[s], s) if s else moved[s]
        part = part.reshape(HELD, ROWS, 1, 2, 4, 8, 128)
        result = lax.dynamic_update_slice_in_dim(result, part, m ^ s, 2)
    return result.transpose(0, 1, 2, 3, 5, 4, 6).reshape(HELD, ROWS, GROUPS * COLS, VALS)


def solution(mesh):
    return jax.shard_map(
        local,
        mesh=mesh,
        in_specs=(
            P("member", "region", None, None),
            P(None, ("member", "region"), None),
            P(None, ("member", "region"), None),
            P(None, ("member", "region"), None),
            P(None, ("member", "region")),
        ),
        out_specs=P("member", "region", None, None),
        check_vma=False,
    )
```

```python
import math

import jax
import jax.numpy as jnp
from jax import lax
from jax.experimental import pallas as pl
from jax.experimental.pallas import tpu as pltpu
from jax.sharding import PartitionSpec as P


SIDE = 16
NS_ITERS = 6
MEMBERS = 24
OBS = 128
VALS = 512
INFLATION_FACTOR = 1.1
INV_SCALE = 1.0 / 288.0

GROUPS = 8
HELD = MEMBERS // GROUPS
ROWS = 2
COLS = 16
BLOCKS = ROWS * COLS
POINTS = 4
EXT_COLS = COLS + 2
FIELD_ROWS = BLOCKS * 4
PITCH = FIELD_ROWS + 4
SLAB = 26
WIDE = 32
SLAB_ROWS = 472
EDGE_PITCH = 20
MAT = MEMBERS + 4
BLOCK_MAT = POINTS * MAT


def first_row(i, c):
    return i * 64 + (c >> 3) * 32 + (c & 7)


def split_bf16(x):
    high = x.astype(jnp.bfloat16)
    low = (x - high.astype(jnp.float32)).astype(jnp.bfloat16)
    return high, low


def observe_kernel(m_ref, *refs):
    parts = refs[:GROUPS]
    obs_ref, west_ref, east_ref, ens_ref, slab0_ref, slab1_ref, edge = refs[GROUPS:]
    slabs = (slab0_ref, slab1_ref)
    m = m_ref[0]
    for s in range(GROUPS):
        for k in range(HELD):
            member = (m ^ s) * HELD + k
            ens_ref[pl.ds(member * PITCH, FIELD_ROWS), :] = parts[s][
                k * FIELD_ROWS : (k + 1) * FIELD_ROWS, :
            ]
            for e in range(2):
                at = HELD * FIELD_ROWS + (e * HELD + k) * 8
                edge[pl.ds(member * EDGE_PITCH + 8 * e, 8), :] = parts[s][at : at + 8, :]

    def one(i, slot, obs, load):
        value = obs[i : i + 1]
        weight = obs[2 + i : 3 + i]
        index_f = obs[4 + i : 5 + i]
        index = jnp.broadcast_to(index_f.astype(jnp.int32), (MEMBERS, OBS))
        lane = index & 127
        chunk = index >> 7
        seen = jnp.zeros((MEMBERS, OBS), jnp.float32)
        for t in range(4):
            got = jnp.take_along_axis(load(t), lane, axis=1, mode="promise_in_bounds")
            seen = jnp.where(chunk == t, got, seen)
        mean = jnp.sum(seen, axis=0, keepdims=True) * (1.0 / MEMBERS)
        base = slot * SLAB
        slabs[i][pl.ds(base, MEMBERS), :] = weight * (seen - mean)
        slabs[i][pl.ds(base + MEMBERS, 1), :] = weight * (value - mean)
        slabs[i][pl.ds(base + MEMBERS + 1, 1), :] = index_f

    def body(c, carry):
        obs = obs_ref[c]
        for i in range(ROWS):
            one(i, c + 1, obs, lambda t: ens_ref[pl.ds(first_row(i, c) + 8 * t, MEMBERS, stride=PITCH), :])
        return carry

    lax.fori_loop(0, COLS, body, 0)
    for e, ref in enumerate((west_ref, east_ref)):
        obs = ref[...]
        for i in range(ROWS):
            one(
                i,
                e * (EXT_COLS - 1),
                obs,
                lambda t: edge[pl.ds(8 * e + 4 * i + t, MEMBERS, stride=EDGE_PITCH), :],
            )


def put_slab(slot, ref, base, source, pair, locs):
    t = lax.broadcasted_iota(jnp.int32, (8, OBS), 0)
    offset = (((t >> 1) - 1) * SIDE - (t & 1) * 8).astype(jnp.float32) - 3.5
    cell = ref[pl.ds(base + MEMBERS + 1, 1), :].astype(jnp.int32) & 255
    dy = (cell >> 4).astype(jnp.float32) + offset
    dx = (cell & 15).astype(jnp.float32) + offset
    locs[slot, 0:8, :] = jnp.exp(-(dy * dy) * INV_SCALE)
    locs[slot, 8:16, :] = jnp.exp(-(dx * dx) * INV_SCALE)
    scaled = ref[pl.ds(base, MEMBERS), :]
    source[slot] = scaled
    innovation = jnp.broadcast_to(ref[pl.ds(base + MEMBERS, 1), :], (8, OBS))
    high, low = split_bf16(jnp.concatenate([scaled, innovation], axis=0))
    pair[slot] = jnp.concatenate([high, low], axis=0)


def contribution(slot, di, dj, source, pair, locs):
    loc = locs[slot]
    base = source[slot]
    rows = []
    for a in range(2):
        for b in range(2):
            w = loc[2 * di + a : 2 * di + a + 1] * loc[8 + 2 * dj + b : 9 + 2 * dj + b]
            rows.append(w * base)
    high, low = split_bf16(jnp.concatenate(rows, axis=0))
    both = pair[slot]
    return lax.dot_general(
        jnp.concatenate([high, low], axis=1),
        jnp.concatenate([both, both], axis=1),
        (((1,), (1,)), ((), ())),
        preferred_element_type=jnp.float32,
    )


def own_gram_kernel(slab0_ref, slab1_ref, gram_ref, source, pair, locs):
    def put(c, carry):
        for i, ref in enumerate((slab0_ref, slab1_ref)):
            put_slab(i * EXT_COLS + c, ref, c * SLAB, source, pair, locs)
        return carry

    lax.fori_loop(0, EXT_COLS, put, 0)

    def one(c, carry):
        for i in range(ROWS):
            acc = jnp.zeros((POINTS * MEMBERS, 2 * WIDE), jnp.float32)
            for q in range(ROWS):
                for dj in range(3):
                    acc = acc + contribution(q * EXT_COLS + c + dj, q - i + 1, dj, source, pair, locs)
            for p in range(POINTS):
                gram_ref[pl.ds((i * COLS + c) * BLOCK_MAT + p * MAT, MEMBERS), 0 : 2 * WIDE] = acc[
                    p * MEMBERS : (p + 1) * MEMBERS
                ]
        return carry

    lax.fori_loop(0, COLS, one, 0)


def sym_product(left, right, out, finish):
    for tile in range(3):
        lo = 8 * tile
        for half in range(2):
            i0 = lo + 4 * half
            acc = [None] * 4
            for k in range(MEMBERS):
                row = right[k * MAT + lo : k * MAT + MEMBERS, :]
                for step in range(4):
                    at = (i0 + step) * MAT + k
                    term = left[at : at + 1, :] * row
                    acc[step] = term if acc[step] is None else acc[step] + term
            for step in range(4):
                i = i0 + step
                row = finish(acc[step], i, lo)
                out[i * MAT + lo : i * MAT + MEMBERS, :] = row
                for j in range(tile + 1, 3):
                    out[pl.ds(8 * j * MAT + i, 8, stride=MAT), :] = row[8 * (j - tile) : 8 * (j - tile) + 8]


def plain(row, i, lo):
    return row


def newton_step(row, i, lo):
    where = lax.broadcasted_iota(jnp.int32, row.shape, 0) + lo
    return jnp.where(where == i, 1.5, 0.0) - 0.5 * row


def analyze_kernel(m_ref, ens_ref, own_ref, above_ref, below_ref, *refs):
    outs = refs[:GROUPS]
    source, pair, locs, gram, ya, yb, za, zb, mm, drive, moved_ref = refs[GROUPS:]
    m = m_ref[0]

    def put(c, carry):
        put_slab(c, above_ref, c * SLAB, source, pair, locs)
        put_slab(EXT_COLS + c, below_ref, c * SLAB, source, pair, locs)
        return carry

    lax.fori_loop(0, EXT_COLS, put, 0)

    def one_gram(c, carry):
        for i in range(ROWS):
            acc = jnp.zeros((POINTS * MEMBERS, 2 * WIDE), jnp.float32)
            for dj in range(3):
                acc = acc + contribution(i * EXT_COLS + c + dj, 2 * i, dj, source, pair, locs)
            for p in range(POINTS):
                at = (i * COLS + c) * BLOCK_MAT + p * MAT
                gram[pl.ds(at, MEMBERS), 0 : 2 * WIDE] = (
                    own_ref[pl.ds(at, MEMBERS), 0 : 2 * WIDE] + acc[p * MEMBERS : (p + 1) * MEMBERS]
                )
        return carry

    lax.fori_loop(0, COLS, one_gram, 0)
    member = lax.broadcasted_iota(jnp.int32, (MEMBERS, 128), 0)
    squares = jnp.zeros((MEMBERS, 128), jnp.float32)
    for k in range(MEMBERS):
        turned = gram[pl.ds(k, 128, stride=MAT), :].T
        total = turned[0:WIDE] + turned[WIDE : 2 * WIDE]
        row = total[0:MEMBERS] + jnp.where(member == k, (MEMBERS - 1) / INFLATION_FACTOR, 0.0)
        drive[k : k + 1, :] = total[MEMBERS : MEMBERS + 1]
        ya[k * MAT : k * MAT + MEMBERS, :] = row
        squares = squares + row * row
    norm = jnp.sqrt(jnp.sum(squares, axis=0, keepdims=True))
    inverse = 1.0 / norm
    for k in range(MEMBERS):
        row = ya[k * MAT : k * MAT + MEMBERS, :] * inverse
        ya[k * MAT : k * MAT + MEMBERS, :] = row
        za[k * MAT : k * MAT + MEMBERS, :] = newton_step(row, k, 0)

    sym_product(ya, za, yb, plain)

    def two_steps(turn, carry):
        sym_product(za, yb, mm, newton_step)
        sym_product(yb, mm, ya, plain)
        sym_product(mm, za, zb, plain)
        sym_product(zb, ya, mm, newton_step)
        sym_product(ya, mm, yb, plain)
        sym_product(mm, zb, za, plain)
        return carry

    lax.fori_loop(0, (NS_ITERS - 2) // 2, two_steps, 0)
    sym_product(za, yb, mm, newton_step)
    sym_product(mm, za, zb, plain)

    scale = 1.0 / jnp.sqrt(norm)
    half_way = jnp.zeros((MEMBERS, 128), jnp.float32)
    for k in range(MEMBERS):
        half_way = half_way + zb[k * MAT : k * MAT + MEMBERS, :] * drive[k : k + 1, :]
    half_way = half_way * scale
    mean_w = jnp.zeros((MEMBERS, 128), jnp.float32)
    for k in range(MEMBERS):
        mean_w = mean_w + zb[k * MAT : k * MAT + MEMBERS, :] * half_way[k : k + 1]
    mean_w = mean_w * scale
    spread = scale * math.sqrt(MEMBERS - 1)
    blank = jnp.zeros((128 - 3 * MEMBERS, 128), jnp.float32)
    for k in range(MEMBERS):
        weight = mean_w + spread * zb[k * MAT : k * MAT + MEMBERS, :]
        high = weight.astype(jnp.bfloat16).astype(jnp.float32)
        gram[pl.ds(k, 128, stride=MAT), :] = jnp.concatenate(
            [high, high, weight - high, blank], axis=0
        ).T

    right_half = (lax.broadcasted_iota(jnp.int32, (MEMBERS, 128), 1) >> 3) & 1

    def one_update(c, carry):
        for i in range(ROWS):
            at = (i * COLS + c) * BLOCK_MAT
            first = first_row(i, c)
            ens = jnp.concatenate(
                [ens_ref[pl.ds(first + 8 * t, MEMBERS, stride=PITCH), :] for t in range(4)], axis=1
            )
            mean = jnp.sum(ens, axis=0, keepdims=True) * (1.0 / MEMBERS)
            anomaly = ens - mean
            high = anomaly.astype(jnp.bfloat16).astype(jnp.float32)
            low = anomaly - high
            stacked = jnp.concatenate(
                [high, low, high, jnp.zeros((128 - 3 * MEMBERS, VALS), jnp.float32)], axis=0
            ).astype(jnp.bfloat16)
            for a in range(2):
                values = jnp.concatenate(
                    [stacked[:, 128 * a : 128 * a + 128], stacked[:, 256 + 128 * a : 384 + 128 * a]], axis=1
                )
                weight = jnp.concatenate(
                    [gram[pl.ds(at + (2 * a + b) * MAT, MEMBERS), :] for b in range(2)], axis=0
                ).astype(jnp.bfloat16)
                moved = jnp.dot(weight, values, preferred_element_type=jnp.float32)
                for f in range(2):
                    part = moved[:, 128 * f : 128 * f + 128]
                    t = 2 * f + a
                    moved_tile = jnp.where(right_half == 1, part[MEMBERS:], part[:MEMBERS])
                    moved_ref[pl.ds(first + 8 * t, MEMBERS, stride=PITCH), :] = (
                        mean[:, 128 * t : 128 * t + 128] + moved_tile
                    )
        return carry

    lax.fori_loop(0, COLS, one_update, 0)
    for s in range(GROUPS):
        for k in range(HELD):
            start = ((m ^ s) * HELD + k) * PITCH
            outs[s][k * FIELD_ROWS : (k + 1) * FIELD_ROWS, :] = moved_ref[pl.ds(start, FIELD_ROWS), :]


def f32(*shape):
    return jax.ShapeDtypeStruct(shape, jnp.float32)


def tables(slots):
    return [
        pltpu.VMEM((slots, MEMBERS, OBS), jnp.float32),
        pltpu.VMEM((slots, 2 * WIDE, OBS), jnp.bfloat16),
        pltpu.VMEM((slots, 16, OBS), jnp.float32),
    ]


def vmem_call(kernel, out_shape, flops, args, scratch=()):
    places = [
        pl.BlockSpec(memory_space=pltpu.SMEM if x.dtype == jnp.int32 else pltpu.VMEM) for x in args
    ]
    return pl.pallas_call(
        kernel,
        out_shape=out_shape,
        in_specs=places,
        scratch_shapes=list(scratch),
        cost_estimate=pl.CostEstimate(flops=flops, bytes_accessed=0, transcendentals=0),
        compiler_params=pltpu.CompilerParams(vmem_limit_bytes=32 * 1024 * 1024),
    )(*args)


def swapped(x, s):
    return lax.ppermute(x, "member", [(a, a ^ s) for a in range(GROUPS)])


def shifted(x, axis, by):
    devices = lax.axis_size(axis)
    pairs = [(i, i + by) for i in range(devices) if 0 <= i + by < devices]
    return lax.ppermute(x, axis, pairs)


def local(ensemble, obs_value, obs_error, obs_index, obs_count):
    m = lax.axis_index("member").astype(jnp.int32)
    where = m.reshape(1)
    tiled = ensemble.reshape(HELD, ROWS, GROUPS, 2, 8, 4, 128).transpose(2, 0, 1, 3, 5, 4, 6)
    parts = []
    for s in range(GROUPS):
        to = m ^ s
        part = lax.dynamic_index_in_dim(tiled, to, 0, keepdims=False)
        edges = [
            lax.dynamic_slice_in_dim(ensemble, jnp.clip(at, 0, GROUPS * COLS - 1), 1, 2)
            for at in (to * COLS - 1, to * COLS + COLS)
        ]
        part = jnp.concatenate([x.reshape(-1, 128) for x in (part, *edges)], axis=0)
        parts.append(swapped(part, s) if s else part)

    slot = lax.broadcasted_iota(jnp.int32, (32, 1, OBS), 2)
    live = jnp.where(slot < obs_count[:, :, None], 1.0, 0.0).astype(jnp.float32)
    root_weight = jnp.sqrt(live / obs_error)
    pieces = [obs_value, root_weight, obs_index.astype(jnp.float32), jnp.zeros_like(obs_value)]
    packed = jnp.concatenate([x.reshape(COLS, ROWS, OBS) for x in pieces], axis=1)
    obs = lax.all_to_all(packed, "region", split_axis=0, concat_axis=0, tiled=True)

    west = shifted(obs[COLS - 1], "member", 1)
    east = shifted(obs[0], "member", -1)

    ens, slab0, slab1 = vmem_call(
        observe_kernel,
        (f32(MEMBERS * PITCH, 128), f32(SLAB_ROWS, OBS), f32(SLAB_ROWS, OBS)),
        10**9,
        [where, *parts, obs, west, east],
        [pltpu.VMEM((MEMBERS * EDGE_PITCH, 128), jnp.float32)],
    )

    below = shifted(slab0, "region", -1)
    above = shifted(slab1, "region", 1)

    own = vmem_call(
        own_gram_kernel,
        f32(BLOCKS * BLOCK_MAT, 128),
        4 * 10**9,
        [slab0, slab1],
        tables(ROWS * EXT_COLS),
    )

    square = pltpu.VMEM((MEMBERS * MAT, 128), jnp.float32)
    moved = vmem_call(
        analyze_kernel,
        [f32(HELD * FIELD_ROWS, 128)] * GROUPS,
        10**10,
        [where, ens, own, above, below],
        tables(ROWS * EXT_COLS)
        + [
            pltpu.VMEM((BLOCKS * BLOCK_MAT, 128), jnp.float32),
            square, square, square, square, square,
            pltpu.VMEM((MEMBERS, 128), jnp.float32),
            pltpu.VMEM((MEMBERS * PITCH, 128), jnp.float32),
        ],
    )

    result = jnp.zeros((HELD, ROWS, GROUPS, 2, 4, 8, 128), jnp.float32)
    for s in range(GROUPS):
        part = swapped(moved[s], s) if s else moved[s]
        part = part.reshape(HELD, ROWS, 1, 2, 4, 8, 128)
        result = lax.dynamic_update_slice_in_dim(result, part, m ^ s, 2)
    return result.transpose(0, 1, 2, 3, 5, 4, 6).reshape(HELD, ROWS, GROUPS * COLS, VALS)


def solution(mesh):
    return jax.shard_map(
        local,
        mesh=mesh,
        in_specs=(
            P("member", "region", None, None),
            P(None, ("member", "region"), None),
            P(None, ("member", "region"), None),
            P(None, ("member", "region"), None),
            P(None, ("member", "region")),
        ),
        out_specs=P("member", "region", None, None),
        check_vma=False,
    )
```

```python
import math

import jax
import jax.numpy as jnp
from jax import lax
from jax.experimental import pallas as pl
from jax.experimental.pallas import tpu as pltpu
from jax.sharding import PartitionSpec as P


SIDE = 16
NS_ITERS = 6
MEMBERS = 24
OBS = 128
VALS = 512
INFLATION_FACTOR = 1.1
INV_SCALE = 1.0 / 288.0

GROUPS = 8
HELD = MEMBERS // GROUPS
ROWS = 2
COLS = 16
BLOCKS = ROWS * COLS
POINTS = 4
EXT_COLS = COLS + 2
FIELD_ROWS = BLOCKS * 4
PITCH = FIELD_ROWS + 4
SLAB = 26
WIDE = 32
STACK = 80
SLAB_ROWS = 472
EDGE_PITCH = 20
MAT = MEMBERS + 4
BLOCK_MAT = POINTS * MAT


def first_row(i, c):
    return i * 64 + (c >> 3) * 32 + (c & 7)


def split_bf16(x):
    high = x.astype(jnp.bfloat16)
    low = (x - high.astype(jnp.float32)).astype(jnp.bfloat16)
    return high, low


def observe_kernel(m_ref, *refs):
    parts = refs[:GROUPS]
    obs_ref, west_ref, east_ref, ens_ref, slab0_ref, slab1_ref, edge = refs[GROUPS:]
    slabs = (slab0_ref, slab1_ref)
    m = m_ref[0]
    for s in range(GROUPS):
        for k in range(HELD):
            member = (m ^ s) * HELD + k
            ens_ref[pl.ds(member * PITCH, FIELD_ROWS), :] = parts[s][
                k * FIELD_ROWS : (k + 1) * FIELD_ROWS, :
            ]
            for e in range(2):
                at = HELD * FIELD_ROWS + (e * HELD + k) * 8
                edge[pl.ds(member * EDGE_PITCH + 8 * e, 8), :] = parts[s][at : at + 8, :]

    def one(i, slot, obs, load):
        value = obs[i : i + 1]
        weight = obs[2 + i : 3 + i]
        index_f = obs[4 + i : 5 + i]
        index = jnp.broadcast_to(index_f.astype(jnp.int32), (MEMBERS, OBS))
        lane = index & 127
        chunk = index >> 7
        seen = jnp.zeros((MEMBERS, OBS), jnp.float32)
        for t in range(4):
            got = jnp.take_along_axis(load(t), lane, axis=1, mode="promise_in_bounds")
            seen = jnp.where(chunk == t, got, seen)
        mean = jnp.sum(seen, axis=0, keepdims=True) * (1.0 / MEMBERS)
        base = slot * SLAB
        slabs[i][pl.ds(base, MEMBERS), :] = weight * (seen - mean)
        slabs[i][pl.ds(base + MEMBERS, 1), :] = weight * (value - mean)
        slabs[i][pl.ds(base + MEMBERS + 1, 1), :] = index_f

    def body(c, carry):
        obs = obs_ref[c]
        for i in range(ROWS):
            one(i, c + 1, obs, lambda t: ens_ref[pl.ds(first_row(i, c) + 8 * t, MEMBERS, stride=PITCH), :])
        return carry

    lax.fori_loop(0, COLS, body, 0, unroll=2)
    for e, ref in enumerate((west_ref, east_ref)):
        obs = ref[...]
        for i in range(ROWS):
            one(
                i,
                e * (EXT_COLS - 1),
                obs,
                lambda t: edge[pl.ds(8 * e + 4 * i + t, MEMBERS, stride=EDGE_PITCH), :],
            )


def put_slab(slot, ref, base, source, pair, locs):
    t = lax.broadcasted_iota(jnp.int32, (8, OBS), 0)
    offset = (((t >> 1) - 1) * SIDE - (t & 1) * 8).astype(jnp.float32) - 3.5
    cell = ref[pl.ds(base + MEMBERS + 1, 1), :].astype(jnp.int32) & 255
    dy = (cell >> 4).astype(jnp.float32) + offset
    dx = (cell & 15).astype(jnp.float32) + offset
    locs[slot, 0:8, :] = jnp.exp(-(dy * dy) * INV_SCALE)
    locs[slot, 8:16, :] = jnp.exp(-(dx * dx) * INV_SCALE)
    scaled = ref[pl.ds(base, MEMBERS), :]
    source[slot] = scaled
    innovation = jnp.broadcast_to(ref[pl.ds(base + MEMBERS, 1), :], (8, OBS))
    high, low = split_bf16(jnp.concatenate([scaled, innovation], axis=0))
    pair[slot] = jnp.concatenate([high, low], axis=0)


def contribution(slot, di, dj, source, pair, locs):
    loc = locs[slot]
    base = source[slot]
    rows = []
    for a in range(2):
        for b in range(2):
            w = loc[2 * di + a : 2 * di + a + 1] * loc[8 + 2 * dj + b : 9 + 2 * dj + b]
            rows.append(w * base)
    high, low = split_bf16(jnp.concatenate(rows, axis=0))
    both = pair[slot]
    return lax.dot_general(
        jnp.concatenate([high, low], axis=1),
        jnp.concatenate([both, both], axis=1),
        (((1,), (1,)), ((), ())),
        preferred_element_type=jnp.float32,
    )


def own_gram_kernel(slab0_ref, slab1_ref, ens_ref, gram_ref, stack_ref, mean_ref, source, pair, locs):
    def put(c, carry):
        for i, ref in enumerate((slab0_ref, slab1_ref)):
            put_slab(i * EXT_COLS + c, ref, c * SLAB, source, pair, locs)
        return carry

    lax.fori_loop(0, EXT_COLS, put, 0)

    def one(c, carry):
        for i in range(ROWS):
            acc = jnp.zeros((POINTS * MEMBERS, 2 * WIDE), jnp.float32)
            for q in range(ROWS):
                for dj in range(3):
                    acc = acc + contribution(q * EXT_COLS + c + dj, q - i + 1, dj, source, pair, locs)
            for p in range(POINTS):
                gram_ref[pl.ds((i * COLS + c) * BLOCK_MAT + p * MAT, MEMBERS), 0 : 2 * WIDE] = acc[
                    p * MEMBERS : (p + 1) * MEMBERS
                ]
        return carry

    lax.fori_loop(0, COLS, one, 0, unroll=4)

    def stack(c, carry):
        for i in range(ROWS):
            block = i * COLS + c
            for t in range(4):
                ens = ens_ref[pl.ds(first_row(i, c) + 8 * t, MEMBERS, stride=PITCH), :]
                mean = jnp.sum(ens, axis=0, keepdims=True) * (1.0 / MEMBERS)
                mean_ref[pl.ds(block * 4 + t, 1), :] = mean
                anomaly = ens - mean
                high = anomaly.astype(jnp.bfloat16).astype(jnp.float32)
                rows = jnp.concatenate(
                    [high, anomaly - high, high, jnp.zeros((STACK - 3 * MEMBERS, 128), jnp.float32)], axis=0
                )
                f, a = t // 2, t % 2
                stack_ref[2 * block + a, :, 128 * f : 128 * f + 128] = rows.astype(jnp.bfloat16)
        return carry

    lax.fori_loop(0, COLS, stack, 0, unroll=2)


def sym_product(left, right, out, finish):
    for tile in range(3):
        lo = 8 * tile
        for half in range(2):
            i0 = lo + 4 * half
            acc = [None] * 4
            for k in range(MEMBERS):
                row = right[k * MAT + lo : k * MAT + MEMBERS, :]
                for step in range(4):
                    at = (i0 + step) * MAT + k
                    term = left[at : at + 1, :] * row
                    acc[step] = term if acc[step] is None else acc[step] + term
            for step in range(4):
                i = i0 + step
                row = finish(acc[step], i, lo)
                out[i * MAT + lo : i * MAT + MEMBERS, :] = row
                for j in range(tile + 1, 3):
                    out[pl.ds(8 * j * MAT + i, 8, stride=MAT), :] = row[8 * (j - tile) : 8 * (j - tile) + 8]


def plain(row, i, lo):
    return row


def newton_step(row, i, lo):
    where = lax.broadcasted_iota(jnp.int32, row.shape, 0) + lo
    return jnp.where(where == i, 1.5, 0.0) - 0.5 * row


def analyze_kernel(m_ref, stack_ref, mean_ref, own_ref, above_ref, below_ref, *refs):
    outs = refs[:GROUPS]
    source, pair, locs, gram, ya, yb, za, zb, mm, drive, moved_ref = refs[GROUPS:]
    m = m_ref[0]

    def put(c, carry):
        put_slab(c, above_ref, c * SLAB, source, pair, locs)
        put_slab(EXT_COLS + c, below_ref, c * SLAB, source, pair, locs)
        return carry

    lax.fori_loop(0, EXT_COLS, put, 0)

    def one_gram(c, carry):
        for i in range(ROWS):
            acc = jnp.zeros((POINTS * MEMBERS, 2 * WIDE), jnp.float32)
            for dj in range(3):
                acc = acc + contribution(i * EXT_COLS + c + dj, 2 * i, dj, source, pair, locs)
            for p in range(POINTS):
                at = (i * COLS + c) * BLOCK_MAT + p * MAT
                gram[pl.ds(at, MEMBERS), 0 : 2 * WIDE] = (
                    own_ref[pl.ds(at, MEMBERS), 0 : 2 * WIDE] + acc[p * MEMBERS : (p + 1) * MEMBERS]
                )
        return carry

    lax.fori_loop(0, COLS, one_gram, 0, unroll=8)
    member = lax.broadcasted_iota(jnp.int32, (MEMBERS, 128), 0)
    squares = jnp.zeros((MEMBERS, 128), jnp.float32)
    for k in range(MEMBERS):
        turned = gram[pl.ds(k, 128, stride=MAT), :].T
        total = turned[0:WIDE] + turned[WIDE : 2 * WIDE]
        row = total[0:MEMBERS] + jnp.where(member == k, (MEMBERS - 1) / INFLATION_FACTOR, 0.0)
        drive[k : k + 1, :] = total[MEMBERS : MEMBERS + 1]
        ya[k * MAT : k * MAT + MEMBERS, :] = row
        squares = squares + row * row
    norm = jnp.sqrt(jnp.sum(squares, axis=0, keepdims=True))
    inverse = 1.0 / norm
    for k in range(MEMBERS):
        row = ya[k * MAT : k * MAT + MEMBERS, :] * inverse
        ya[k * MAT : k * MAT + MEMBERS, :] = row
        za[k * MAT : k * MAT + MEMBERS, :] = newton_step(row, k, 0)

    sym_product(ya, za, yb, plain)

    def two_steps(turn, carry):
        sym_product(za, yb, mm, newton_step)
        sym_product(yb, mm, ya, plain)
        sym_product(mm, za, zb, plain)
        sym_product(zb, ya, mm, newton_step)
        sym_product(ya, mm, yb, plain)
        sym_product(mm, zb, za, plain)
        return carry

    lax.fori_loop(0, (NS_ITERS - 2) // 2, two_steps, 0)
    sym_product(za, yb, mm, newton_step)
    sym_product(mm, za, zb, plain)

    scale = 1.0 / jnp.sqrt(norm)
    half_way = jnp.zeros((MEMBERS, 128), jnp.float32)
    for k in range(MEMBERS):
        half_way = half_way + zb[k * MAT : k * MAT + MEMBERS, :] * drive[k : k + 1, :]
    half_way = half_way * scale
    mean_w = jnp.zeros((MEMBERS, 128), jnp.float32)
    for k in range(MEMBERS):
        mean_w = mean_w + zb[k * MAT : k * MAT + MEMBERS, :] * half_way[k : k + 1]
    mean_w = mean_w * scale
    spread = scale * math.sqrt(MEMBERS - 1)
    blank = jnp.zeros((128 - 3 * MEMBERS, 128), jnp.float32)
    for k in range(MEMBERS):
        weight = mean_w + spread * zb[k * MAT : k * MAT + MEMBERS, :]
        high = weight.astype(jnp.bfloat16).astype(jnp.float32)
        gram[pl.ds(k, 128, stride=MAT), :] = jnp.concatenate(
            [high, high, weight - high, blank], axis=0
        ).T

    right_half = (lax.broadcasted_iota(jnp.int32, (MEMBERS, 128), 1) >> 3) & 1

    def one_update(c, carry):
        for i in range(ROWS):
            at = (i * COLS + c) * BLOCK_MAT
            first = first_row(i, c)
            for a in range(2):
                values = jnp.concatenate(
                    [stack_ref[2 * (i * COLS + c) + a], jnp.zeros((128 - STACK, 256), jnp.bfloat16)], axis=0
                )
                weight = jnp.concatenate(
                    [gram[pl.ds(at + (2 * a + b) * MAT, MEMBERS), :] for b in range(2)], axis=0
                ).astype(jnp.bfloat16)
                moved = jnp.dot(weight, values, preferred_element_type=jnp.float32)
                for f in range(2):
                    part = moved[:, 128 * f : 128 * f + 128]
                    t = 2 * f + a
                    moved_tile = jnp.where(right_half == 1, part[MEMBERS:], part[:MEMBERS])
                    moved_ref[pl.ds(first + 8 * t, MEMBERS, stride=PITCH), :] = (
                        mean_ref[pl.ds((i * COLS + c) * 4 + t, 1), :] + moved_tile
                    )
        return carry

    lax.fori_loop(0, COLS, one_update, 0, unroll=8)
    for s in range(GROUPS):
        for k in range(HELD):
            start = ((m ^ s) * HELD + k) * PITCH
            outs[s][k * FIELD_ROWS : (k + 1) * FIELD_ROWS, :] = moved_ref[pl.ds(start, FIELD_ROWS), :]


def f32(*shape):
    return jax.ShapeDtypeStruct(shape, jnp.float32)


def tables(slots):
    return [
        pltpu.VMEM((slots, MEMBERS, OBS), jnp.float32),
        pltpu.VMEM((slots, 2 * WIDE, OBS), jnp.bfloat16),
        pltpu.VMEM((slots, 16, OBS), jnp.float32),
    ]


def vmem_call(kernel, out_shape, flops, args, scratch=()):
    places = [
        pl.BlockSpec(memory_space=pltpu.SMEM if x.dtype == jnp.int32 else pltpu.VMEM) for x in args
    ]
    return pl.pallas_call(
        kernel,
        out_shape=out_shape,
        in_specs=places,
        scratch_shapes=list(scratch),
        cost_estimate=pl.CostEstimate(flops=flops, bytes_accessed=0, transcendentals=0),
        compiler_params=pltpu.CompilerParams(vmem_limit_bytes=32 * 1024 * 1024),
    )(*args)


def swapped(x, s):
    return lax.ppermute(x, "member", [(a, a ^ s) for a in range(GROUPS)])


def shifted(x, axis, by):
    devices = lax.axis_size(axis)
    pairs = [(i, i + by) for i in range(devices) if 0 <= i + by < devices]
    return lax.ppermute(x, axis, pairs)


def local(ensemble, obs_value, obs_error, obs_index, obs_count):
    m = lax.axis_index("member").astype(jnp.int32)
    where = m.reshape(1)
    tiled = ensemble.reshape(HELD, ROWS, GROUPS, 2, 8, 4, 128).transpose(2, 0, 1, 3, 5, 4, 6)
    parts = []
    for s in range(GROUPS):
        to = m ^ s
        part = lax.dynamic_index_in_dim(tiled, to, 0, keepdims=False)
        edges = [
            lax.dynamic_slice_in_dim(ensemble, jnp.clip(at, 0, GROUPS * COLS - 1), 1, 2)
            for at in (to * COLS - 1, to * COLS + COLS)
        ]
        part = jnp.concatenate([x.reshape(-1, 128) for x in (part, *edges)], axis=0)
        parts.append(swapped(part, s) if s else part)

    slot = lax.broadcasted_iota(jnp.int32, (32, 1, OBS), 2)
    live = jnp.where(slot < obs_count[:, :, None], 1.0, 0.0).astype(jnp.float32)
    root_weight = jnp.sqrt(live / obs_error)
    pieces = [obs_value, root_weight, obs_index.astype(jnp.float32), jnp.zeros_like(obs_value)]
    packed = jnp.concatenate([x.reshape(COLS, ROWS, OBS) for x in pieces], axis=1)
    obs = lax.all_to_all(packed, "region", split_axis=0, concat_axis=0, tiled=True)

    west = shifted(obs[COLS - 1], "member", 1)
    east = shifted(obs[0], "member", -1)

    ens, slab0, slab1 = vmem_call(
        observe_kernel,
        (f32(MEMBERS * PITCH, 128), f32(SLAB_ROWS, OBS), f32(SLAB_ROWS, OBS)),
        10**9,
        [where, *parts, obs, west, east],
        [pltpu.VMEM((MEMBERS * EDGE_PITCH, 128), jnp.float32)],
    )

    below = shifted(slab0, "region", -1)
    above = shifted(slab1, "region", 1)

    own, stack, mean = vmem_call(
        own_gram_kernel,
        (
            f32(BLOCKS * BLOCK_MAT, 128),
            jax.ShapeDtypeStruct((2 * BLOCKS, STACK, 256), jnp.bfloat16),
            f32(BLOCKS * 4, 128),
        ),
        4 * 10**9,
        [slab0, slab1, ens],
        tables(ROWS * EXT_COLS),
    )

    square = pltpu.VMEM((MEMBERS * MAT, 128), jnp.float32)
    moved = vmem_call(
        analyze_kernel,
        [f32(HELD * FIELD_ROWS, 128)] * GROUPS,
        10**10,
        [where, stack, mean, own, above, below],
        tables(ROWS * EXT_COLS)
        + [
            pltpu.VMEM((BLOCKS * BLOCK_MAT, 128), jnp.float32),
            square, square, square, square, square,
            pltpu.VMEM((MEMBERS, 128), jnp.float32),
            pltpu.VMEM((MEMBERS * PITCH, 128), jnp.float32),
        ],
    )

    result = jnp.zeros((HELD, ROWS, GROUPS, 2, 4, 8, 128), jnp.float32)
    for s in range(GROUPS):
        part = swapped(moved[s], s) if s else moved[s]
        part = part.reshape(HELD, ROWS, 1, 2, 4, 8, 128)
        result = lax.dynamic_update_slice_in_dim(result, part, m ^ s, 2)
    return result.transpose(0, 1, 2, 3, 5, 4, 6).reshape(HELD, ROWS, GROUPS * COLS, VALS)


def solution(mesh):
    return jax.shard_map(
        local,
        mesh=mesh,
        in_specs=(
            P("member", "region", None, None),
            P(None, ("member", "region"), None),
            P(None, ("member", "region"), None),
            P(None, ("member", "region"), None),
            P(None, ("member", "region")),
        ),
        out_specs=P("member", "region", None, None),
        check_vma=False,
    )
```

```python
import math

import jax
import jax.numpy as jnp
from jax import lax
from jax.experimental import pallas as pl
from jax.experimental.pallas import tpu as pltpu
from jax.sharding import PartitionSpec as P


SIDE = 16
NS_ITERS = 6
MEMBERS = 24
OBS = 128
VALS = 512
INFLATION_FACTOR = 1.1
INV_SCALE = 1.0 / 288.0

GROUPS = 8
HELD = MEMBERS // GROUPS
ROWS = 2
COLS = 16
BLOCKS = ROWS * COLS
POINTS = 4
EXT_COLS = COLS + 2
FIELD_ROWS = BLOCKS * 4
PITCH = FIELD_ROWS + 4
SLAB = 26
WIDE = 32
STACK = 80
SLAB_ROWS = 472
EDGE_PITCH = 20
PART_ROWS = HELD * (FIELD_ROWS + 16)
MAT = MEMBERS + 4
BLOCK_MAT = POINTS * MAT


def first_row(i, c):
    return i * 64 + (c >> 3) * 32 + (c & 7)


def split_bf16(x):
    high = x.astype(jnp.bfloat16)
    low = (x - high.astype(jnp.float32)).astype(jnp.bfloat16)
    return high, low


def pack_kernel(m_ref, ens_ref, *refs):
    outs = refs[:GROUPS]
    stage, sems = refs[GROUPS:]
    m = m_ref[0]
    tiles = GROUPS * 8
    chunk_rows = tiles * 8
    copies = []
    for n in range(HELD * ROWS):
        copy = pltpu.make_async_copy(
            ens_ref.at[pl.ds(n * chunk_rows, chunk_rows), :],
            stage.at[pl.ds(n * chunk_rows, chunk_rows), :],
            sems.at[n],
        )
        copy.start()
        copies.append(copy)

    for n in range(HELD * ROWS):
        k, i = n // ROWS, n % ROWS
        copies[n].wait()
        for s in range(GROUPS):
            to = m ^ s
            start = pl.multiple_of(n * chunk_rows + to * 64, 64)
            outs[s][n * 64 : n * 64 + 64, :] = stage[pl.ds(start, 64), :]
            before = jnp.maximum(2 * to - 1, 0) * 32 + 7
            after = jnp.minimum(2 * to + 2, 2 * GROUPS - 1) * 32
            for e, at in enumerate((before, after)):
                row = HELD * FIELD_ROWS + (e * HELD + k) * 8 + 4 * i
                outs[s][row : row + 4, :] = stage[pl.ds(n * chunk_rows + at, 4, stride=8), :]


def observe_kernel(m_ref, *refs):
    parts = refs[:GROUPS]
    obs_ref, ens_ref, slab0_ref, slab1_ref, edge = refs[GROUPS:]
    slabs = (slab0_ref, slab1_ref)
    m = m_ref[0]
    for s in range(GROUPS):
        for k in range(HELD):
            member = (m ^ s) * HELD + k
            ens_ref[pl.ds(member * PITCH, FIELD_ROWS), :] = parts[s][
                k * FIELD_ROWS : (k + 1) * FIELD_ROWS, :
            ]
            for e in range(2):
                at = HELD * FIELD_ROWS + (e * HELD + k) * 8
                edge[pl.ds(member * EDGE_PITCH + 8 * e, 8), :] = parts[s][at : at + 8, :]

    def one(i, slot, obs, load):
        value = obs[i : i + 1]
        weight = obs[2 + i : 3 + i]
        index_f = obs[4 + i : 5 + i]
        index = jnp.broadcast_to(index_f.astype(jnp.int32), (MEMBERS, OBS))
        lane = index & 127
        chunk = index >> 7
        seen = jnp.zeros((MEMBERS, OBS), jnp.float32)
        for t in range(4):
            got = jnp.take_along_axis(load(t), lane, axis=1, mode="promise_in_bounds")
            seen = jnp.where(chunk == t, got, seen)
        mean = jnp.sum(seen, axis=0, keepdims=True) * (1.0 / MEMBERS)
        base = slot * SLAB
        slabs[i][pl.ds(base, MEMBERS), :] = weight * (seen - mean)
        slabs[i][pl.ds(base + MEMBERS, 1), :] = weight * (value - mean)
        slabs[i][pl.ds(base + MEMBERS + 1, 1), :] = index_f

    def body(c, carry):
        obs = obs_ref[c]
        for i in range(ROWS):
            one(i, c + 1, obs, lambda t: ens_ref[pl.ds(first_row(i, c) + 8 * t, MEMBERS, stride=PITCH), :])
        return carry

    lax.fori_loop(0, COLS, body, 0, unroll=2)
    for e, source in enumerate((COLS - 1, 0)):
        obs = obs_ref[source, 8:16, :]
        for i in range(ROWS):
            one(
                i,
                e * (EXT_COLS - 1),
                obs,
                lambda t: edge[pl.ds(8 * e + 4 * i + t, MEMBERS, stride=EDGE_PITCH), :],
            )


def put_slab(slot, ref, base, source, pair, locs):
    t = lax.broadcasted_iota(jnp.int32, (8, OBS), 0)
    offset = (((t >> 1) - 1) * SIDE - (t & 1) * 8).astype(jnp.float32) - 3.5
    cell = ref[pl.ds(base + MEMBERS + 1, 1), :].astype(jnp.int32) & 255
    dy = (cell >> 4).astype(jnp.float32) + offset
    dx = (cell & 15).astype(jnp.float32) + offset
    locs[slot, 0:8, :] = jnp.exp(-(dy * dy) * INV_SCALE)
    locs[slot, 8:16, :] = jnp.exp(-(dx * dx) * INV_SCALE)
    scaled = ref[pl.ds(base, MEMBERS), :]
    source[slot] = scaled
    innovation = jnp.broadcast_to(ref[pl.ds(base + MEMBERS, 1), :], (8, OBS))
    high, low = split_bf16(jnp.concatenate([scaled, innovation], axis=0))
    pair[slot] = jnp.concatenate([high, low], axis=0)


def contribution(slot, di, dj, source, pair, locs):
    loc = locs[slot]
    base = source[slot]
    rows = []
    for a in range(2):
        for b in range(2):
            w = loc[2 * di + a : 2 * di + a + 1] * loc[8 + 2 * dj + b : 9 + 2 * dj + b]
            rows.append(w * base)
    high, low = split_bf16(jnp.concatenate(rows, axis=0))
    both = pair[slot]
    return lax.dot_general(
        jnp.concatenate([high, low], axis=1),
        jnp.concatenate([both, both], axis=1),
        (((1,), (1,)), ((), ())),
        preferred_element_type=jnp.float32,
    )


def own_gram_kernel(slab0_ref, slab1_ref, ens_ref, gram_ref, stack_ref, mean_ref, source, pair, locs):
    def put(c, carry):
        for i, ref in enumerate((slab0_ref, slab1_ref)):
            put_slab(i * EXT_COLS + c, ref, c * SLAB, source, pair, locs)
        return carry

    lax.fori_loop(0, EXT_COLS, put, 0)

    def one(c, carry):
        for i in range(ROWS):
            acc = jnp.zeros((POINTS * MEMBERS, 2 * WIDE), jnp.float32)
            for q in range(ROWS):
                for dj in range(3):
                    acc = acc + contribution(q * EXT_COLS + c + dj, q - i + 1, dj, source, pair, locs)
            for p in range(POINTS):
                gram_ref[pl.ds((i * COLS + c) * BLOCK_MAT + p * MAT, MEMBERS), 0 : 2 * WIDE] = acc[
                    p * MEMBERS : (p + 1) * MEMBERS
                ]
        return carry

    lax.fori_loop(0, COLS, one, 0, unroll=4)

    def stack(c, carry):
        for i in range(ROWS):
            block = i * COLS + c
            for t in range(4):
                ens = ens_ref[pl.ds(first_row(i, c) + 8 * t, MEMBERS, stride=PITCH), :]
                mean = jnp.sum(ens, axis=0, keepdims=True) * (1.0 / MEMBERS)
                mean_ref[pl.ds(block * 4 + t, 1), :] = mean
                anomaly = ens - mean
                high = anomaly.astype(jnp.bfloat16).astype(jnp.float32)
                rows = jnp.concatenate(
                    [high, anomaly - high, high, jnp.zeros((STACK - 3 * MEMBERS, 128), jnp.float32)], axis=0
                )
                f, a = t // 2, t % 2
                stack_ref[2 * block + a, :, 128 * f : 128 * f + 128] = rows.astype(jnp.bfloat16)
        return carry

    lax.fori_loop(0, COLS, stack, 0, unroll=2)


def sym_product(left, right, out, finish):
    for tile in range(3):
        lo = 8 * tile
        for half in range(2):
            i0 = lo + 4 * half
            acc = [None] * 4
            for k in range(MEMBERS):
                row = right[k * MAT + lo : k * MAT + MEMBERS, :]
                for step in range(4):
                    at = (i0 + step) * MAT + k
                    term = left[at : at + 1, :] * row
                    acc[step] = term if acc[step] is None else acc[step] + term
            for step in range(4):
                i = i0 + step
                row = finish(acc[step], i, lo)
                out[i * MAT + lo : i * MAT + MEMBERS, :] = row
                for j in range(tile + 1, 3):
                    out[pl.ds(8 * j * MAT + i, 8, stride=MAT), :] = row[8 * (j - tile) : 8 * (j - tile) + 8]


def plain(row, i, lo):
    return row


def newton_step(row, i, lo):
    where = lax.broadcasted_iota(jnp.int32, row.shape, 0) + lo
    return jnp.where(where == i, 1.5, 0.0) - 0.5 * row


def analyze_kernel(m_ref, stack_ref, mean_ref, own_ref, above_ref, below_ref, *refs):
    outs = refs[:GROUPS]
    source, pair, locs, gram, ya, yb, za, zb, mm, drive, moved_ref = refs[GROUPS:]
    m = m_ref[0]

    def put(c, carry):
        put_slab(c, above_ref, c * SLAB, source, pair, locs)
        put_slab(EXT_COLS + c, below_ref, c * SLAB, source, pair, locs)
        return carry

    lax.fori_loop(0, EXT_COLS, put, 0)

    def one_gram(c, carry):
        for i in range(ROWS):
            acc = jnp.zeros((POINTS * MEMBERS, 2 * WIDE), jnp.float32)
            for dj in range(3):
                acc = acc + contribution(i * EXT_COLS + c + dj, 2 * i, dj, source, pair, locs)
            for p in range(POINTS):
                at = (i * COLS + c) * BLOCK_MAT + p * MAT
                gram[pl.ds(at, MEMBERS), 0 : 2 * WIDE] = (
                    own_ref[pl.ds(at, MEMBERS), 0 : 2 * WIDE] + acc[p * MEMBERS : (p + 1) * MEMBERS]
                )
        return carry

    lax.fori_loop(0, COLS, one_gram, 0, unroll=8)
    member = lax.broadcasted_iota(jnp.int32, (MEMBERS, 128), 0)
    squares = jnp.zeros((MEMBERS, 128), jnp.float32)
    for k in range(MEMBERS):
        turned = gram[pl.ds(k, 128, stride=MAT), :].T
        total = turned[0:WIDE] + turned[WIDE : 2 * WIDE]
        row = total[0:MEMBERS] + jnp.where(member == k, (MEMBERS - 1) / INFLATION_FACTOR, 0.0)
        drive[k : k + 1, :] = total[MEMBERS : MEMBERS + 1]
        ya[k * MAT : k * MAT + MEMBERS, :] = row
        squares = squares + row * row
    norm = jnp.sqrt(jnp.sum(squares, axis=0, keepdims=True))
    inverse = 1.0 / norm
    for k in range(MEMBERS):
        row = ya[k * MAT : k * MAT + MEMBERS, :] * inverse
        ya[k * MAT : k * MAT + MEMBERS, :] = row
        za[k * MAT : k * MAT + MEMBERS, :] = newton_step(row, k, 0)

    sym_product(ya, za, yb, plain)

    def two_steps(turn, carry):
        sym_product(za, yb, mm, newton_step)
        sym_product(yb, mm, ya, plain)
        sym_product(mm, za, zb, plain)
        sym_product(zb, ya, mm, newton_step)
        sym_product(ya, mm, yb, plain)
        sym_product(mm, zb, za, plain)
        return carry

    lax.fori_loop(0, (NS_ITERS - 2) // 2, two_steps, 0)
    sym_product(za, yb, mm, newton_step)
    sym_product(mm, za, zb, plain)

    scale = 1.0 / jnp.sqrt(norm)
    half_way = jnp.zeros((MEMBERS, 128), jnp.float32)
    for k in range(MEMBERS):
        half_way = half_way + zb[k * MAT : k * MAT + MEMBERS, :] * drive[k : k + 1, :]
    half_way = half_way * scale
    mean_w = jnp.zeros((MEMBERS, 128), jnp.float32)
    for k in range(MEMBERS):
        mean_w = mean_w + zb[k * MAT : k * MAT + MEMBERS, :] * half_way[k : k + 1]
    mean_w = mean_w * scale
    spread = scale * math.sqrt(MEMBERS - 1)
    blank = jnp.zeros((128 - 3 * MEMBERS, 128), jnp.float32)
    for k in range(MEMBERS):
        weight = mean_w + spread * zb[k * MAT : k * MAT + MEMBERS, :]
        high = weight.astype(jnp.bfloat16).astype(jnp.float32)
        gram[pl.ds(k, 128, stride=MAT), :] = jnp.concatenate(
            [high, high, weight - high, blank], axis=0
        ).T

    right_half = (lax.broadcasted_iota(jnp.int32, (MEMBERS, 128), 1) >> 3) & 1

    def one_update(c, carry):
        for i in range(ROWS):
            at = (i * COLS + c) * BLOCK_MAT
            first = first_row(i, c)
            for a in range(2):
                values = jnp.concatenate(
                    [stack_ref[2 * (i * COLS + c) + a], jnp.zeros((128 - STACK, 256), jnp.bfloat16)], axis=0
                )
                weight = jnp.concatenate(
                    [gram[pl.ds(at + (2 * a + b) * MAT, MEMBERS), :] for b in range(2)], axis=0
                ).astype(jnp.bfloat16)
                moved = jnp.dot(weight, values, preferred_element_type=jnp.float32)
                for f in range(2):
                    part = moved[:, 128 * f : 128 * f + 128]
                    t = 2 * f + a
                    moved_tile = jnp.where(right_half == 1, part[MEMBERS:], part[:MEMBERS])
                    moved_ref[pl.ds(first + 8 * t, MEMBERS, stride=PITCH), :] = (
                        mean_ref[pl.ds((i * COLS + c) * 4 + t, 1), :] + moved_tile
                    )
        return carry

    lax.fori_loop(0, COLS, one_update, 0, unroll=8)
    for s in range(GROUPS):
        for k in range(HELD):
            start = ((m ^ s) * HELD + k) * PITCH
            outs[s][k * FIELD_ROWS : (k + 1) * FIELD_ROWS, :] = moved_ref[pl.ds(start, FIELD_ROWS), :]


def f32(*shape):
    return jax.ShapeDtypeStruct(shape, jnp.float32)


def tables(slots):
    return [
        pltpu.VMEM((slots, MEMBERS, OBS), jnp.float32),
        pltpu.VMEM((slots, 2 * WIDE, OBS), jnp.bfloat16),
        pltpu.VMEM((slots, 16, OBS), jnp.float32),
    ]


def vmem_call(kernel, out_shape, flops, args, scratch=()):
    places = [
        pl.BlockSpec(memory_space=pltpu.SMEM if x.dtype == jnp.int32 else pltpu.VMEM) for x in args
    ]
    return pl.pallas_call(
        kernel,
        out_shape=out_shape,
        in_specs=places,
        scratch_shapes=list(scratch),
        cost_estimate=pl.CostEstimate(flops=flops, bytes_accessed=0, transcendentals=0),
        compiler_params=pltpu.CompilerParams(vmem_limit_bytes=32 * 1024 * 1024),
    )(*args)


def swapped(x, s):
    return lax.ppermute(x, "member", [(a, a ^ s) for a in range(GROUPS)])


def shifted(x, axis, by):
    devices = lax.axis_size(axis)
    pairs = [(i, i + by) for i in range(devices) if 0 <= i + by < devices]
    return lax.ppermute(x, axis, pairs)


def edge_columns(x):
    members, regions = lax.axis_size("member"), lax.axis_size("region")
    pairs = []
    for a in range(members - 1):
        pairs.append((a * regions + regions - 1, (a + 1) * regions + regions - 1))
        pairs.append(((a + 1) * regions, a * regions))
    return lax.ppermute(x, ("member", "region"), pairs)


def local(ensemble, obs_value, obs_error, obs_index, obs_count):
    m = lax.axis_index("member").astype(jnp.int32)
    where = m.reshape(1)
    tiled = ensemble.reshape(HELD, ROWS, 2 * GROUPS, 8, 4, 128).transpose(0, 1, 2, 4, 3, 5).reshape(-1, 128)
    pieces = pl.pallas_call(
        pack_kernel,
        out_shape=[f32(PART_ROWS, 128)] * GROUPS,
        in_specs=[pl.BlockSpec(memory_space=pltpu.SMEM), pl.BlockSpec(memory_space=pltpu.HBM)],
        scratch_shapes=[
            pltpu.VMEM((HELD * ROWS * GROUPS * 64, 128), jnp.float32),
            pltpu.SemaphoreType.DMA((HELD * ROWS,)),
        ],
        compiler_params=pltpu.CompilerParams(vmem_limit_bytes=54000000),
    )(where, tiled)
    slot = lax.broadcasted_iota(jnp.int32, (32, 1, OBS), 2)
    live = jnp.where(slot < obs_count[:, :, None], 1.0, 0.0).astype(jnp.float32)
    root_weight = jnp.sqrt(live / obs_error)
    columns = [obs_value, root_weight, obs_index.astype(jnp.float32), jnp.zeros_like(obs_value)]
    packed = jnp.concatenate([x.reshape(COLS, ROWS, OBS) for x in columns], axis=1)
    beside = edge_columns(packed)
    packed = jnp.concatenate([packed, beside], axis=1)
    parts = [swapped(pieces[s], s) if s else pieces[s] for s in range(GROUPS)]

    obs = lax.all_to_all(packed, "region", split_axis=0, concat_axis=0, tiled=True)

    ens, slab0, slab1 = vmem_call(
        observe_kernel,
        (f32(MEMBERS * PITCH, 128), f32(SLAB_ROWS, OBS), f32(SLAB_ROWS, OBS)),
        10**9,
        [where, *parts, obs],
        [pltpu.VMEM((MEMBERS * EDGE_PITCH, 128), jnp.float32)],
    )

    below = shifted(slab0, "region", -1)
    above = shifted(slab1, "region", 1)

    own, stack, mean = vmem_call(
        own_gram_kernel,
        (
            f32(BLOCKS * BLOCK_MAT, 128),
            jax.ShapeDtypeStruct((2 * BLOCKS, STACK, 256), jnp.bfloat16),
            f32(BLOCKS * 4, 128),
        ),
        4 * 10**9,
        [slab0, slab1, ens],
        tables(ROWS * EXT_COLS),
    )

    square = pltpu.VMEM((MEMBERS * MAT, 128), jnp.float32)
    moved = vmem_call(
        analyze_kernel,
        [f32(HELD * FIELD_ROWS, 128)] * GROUPS,
        10**10,
        [where, stack, mean, own, above, below],
        tables(ROWS * EXT_COLS)
        + [
            pltpu.VMEM((BLOCKS * BLOCK_MAT, 128), jnp.float32),
            square, square, square, square, square,
            pltpu.VMEM((MEMBERS, 128), jnp.float32),
            pltpu.VMEM((MEMBERS * PITCH, 128), jnp.float32),
        ],
    )

    result = jnp.zeros((HELD, ROWS, GROUPS, 2, 4, 8, 128), jnp.float32)
    for s in range(GROUPS):
        part = swapped(moved[s], s) if s else moved[s]
        part = part.reshape(HELD, ROWS, 1, 2, 4, 8, 128)
        result = lax.dynamic_update_slice_in_dim(result, part, m ^ s, 2)
    return result.transpose(0, 1, 2, 3, 5, 4, 6).reshape(HELD, ROWS, GROUPS * COLS, VALS)


def solution(mesh):
    return jax.shard_map(
        local,
        mesh=mesh,
        in_specs=(
            P("member", "region", None, None),
            P(None, ("member", "region"), None),
            P(None, ("member", "region"), None),
            P(None, ("member", "region"), None),
            P(None, ("member", "region")),
        ),
        out_specs=P("member", "region", None, None),
        check_vma=False,
    )
```

```python
import math

import jax
import jax.numpy as jnp
from jax import lax
from jax.experimental import pallas as pl
from jax.experimental.pallas import tpu as pltpu
from jax.sharding import PartitionSpec as P


SIDE = 16
NS_ITERS = 6
MEMBERS = 24
OBS = 128
VALS = 512
INFLATION_FACTOR = 1.1
INV_SCALE = 1.0 / 288.0

GROUPS = 8
HELD = MEMBERS // GROUPS
ROWS = 2
COLS = 16
BLOCKS = ROWS * COLS
POINTS = 4
EXT_COLS = COLS + 2
FIELD_ROWS = BLOCKS * 4
PITCH = FIELD_ROWS + 4
SLAB = 26
WIDE = 32
STACK = 80
SLAB_ROWS = 472
EDGE_PITCH = 20
PART_ROWS = HELD * (FIELD_ROWS + 16)
MAT = MEMBERS + 4
BLOCK_MAT = POINTS * MAT


def first_row(i, c):
    return i * 64 + (c >> 3) * 32 + (c & 7)


def split_bf16(x):
    high = x.astype(jnp.bfloat16)
    low = (x - high.astype(jnp.float32)).astype(jnp.bfloat16)
    return high, low


def pack_kernel(m_ref, ens_ref, *refs):
    outs = refs[:GROUPS]
    stage, sems = refs[GROUPS:]
    m = m_ref[0]
    tiles = GROUPS * 8
    chunk_rows = tiles * 8
    copies = []
    for n in range(HELD * ROWS):
        copy = pltpu.make_async_copy(
            ens_ref.at[pl.ds(n * chunk_rows, chunk_rows), :],
            stage.at[pl.ds(n * chunk_rows, chunk_rows), :],
            sems.at[n],
        )
        copy.start()
        copies.append(copy)

    for n in range(HELD * ROWS):
        k, i = n // ROWS, n % ROWS
        copies[n].wait()
        for s in range(GROUPS):
            to = m ^ s
            start = pl.multiple_of(n * chunk_rows + to * 64, 64)
            outs[s][n * 64 : n * 64 + 64, :] = stage[pl.ds(start, 64), :]
            before = jnp.maximum(2 * to - 1, 0) * 32 + 7
            after = jnp.minimum(2 * to + 2, 2 * GROUPS - 1) * 32
            for e, at in enumerate((before, after)):
                row = HELD * FIELD_ROWS + (e * HELD + k) * 8 + 4 * i
                outs[s][row : row + 4, :] = stage[pl.ds(n * chunk_rows + at, 4, stride=8), :]


def observe_kernel(m_ref, *refs):
    parts = refs[:GROUPS]
    obs_ref, ens_ref, slab0_ref, slab1_ref, edge = refs[GROUPS:]
    slabs = (slab0_ref, slab1_ref)
    m = m_ref[0]
    for s in range(GROUPS):
        for k in range(HELD):
            member = (m ^ s) * HELD + k
            ens_ref[pl.ds(member * PITCH, FIELD_ROWS), :] = parts[s][
                k * FIELD_ROWS : (k + 1) * FIELD_ROWS, :
            ]
            for e in range(2):
                at = HELD * FIELD_ROWS + (e * HELD + k) * 8
                edge[pl.ds(member * EDGE_PITCH + 8 * e, 8), :] = parts[s][at : at + 8, :]

    def one(i, slot, obs, load):
        value = obs[i : i + 1]
        weight = obs[2 + i : 3 + i]
        index_f = obs[4 + i : 5 + i]
        index = jnp.broadcast_to(index_f.astype(jnp.int32), (MEMBERS, OBS))
        lane = index & 127
        chunk = index >> 7
        seen = jnp.zeros((MEMBERS, OBS), jnp.float32)
        for t in range(4):
            got = jnp.take_along_axis(load(t), lane, axis=1, mode="promise_in_bounds")
            seen = jnp.where(chunk == t, got, seen)
        mean = jnp.sum(seen, axis=0, keepdims=True) * (1.0 / MEMBERS)
        base = slot * SLAB
        slabs[i][pl.ds(base, MEMBERS), :] = weight * (seen - mean)
        slabs[i][pl.ds(base + MEMBERS, 1), :] = weight * (value - mean)
        slabs[i][pl.ds(base + MEMBERS + 1, 1), :] = index_f

    def body(c, carry):
        obs = obs_ref[c]
        for i in range(ROWS):
            one(i, c + 1, obs, lambda t: ens_ref[pl.ds(first_row(i, c) + 8 * t, MEMBERS, stride=PITCH), :])
        return carry

    lax.fori_loop(0, COLS, body, 0, unroll=2)
    for e, source in enumerate((COLS - 1, 0)):
        obs = obs_ref[source, 8:16, :]
        for i in range(ROWS):
            one(
                i,
                e * (EXT_COLS - 1),
                obs,
                lambda t: edge[pl.ds(8 * e + 4 * i + t, MEMBERS, stride=EDGE_PITCH), :],
            )


def put_slab(slot, ref, base, source, pair, locs):
    t = lax.broadcasted_iota(jnp.int32, (8, OBS), 0)
    offset = (((t >> 1) - 1) * SIDE - (t & 1) * 8).astype(jnp.float32) - 3.5
    cell = ref[pl.ds(base + MEMBERS + 1, 1), :].astype(jnp.int32) & 255
    dy = (cell >> 4).astype(jnp.float32) + offset
    dx = (cell & 15).astype(jnp.float32) + offset
    locs[slot, 0:8, :] = jnp.exp(-(dy * dy) * INV_SCALE)
    locs[slot, 8:16, :] = jnp.exp(-(dx * dx) * INV_SCALE)
    scaled = ref[pl.ds(base, MEMBERS), :]
    source[slot] = scaled
    innovation = jnp.broadcast_to(ref[pl.ds(base + MEMBERS, 1), :], (8, OBS))
    high, low = split_bf16(jnp.concatenate([scaled, innovation], axis=0))
    pair[slot] = jnp.concatenate([high, low], axis=0)


def contribution(slot, di, dj, source, pair, locs):
    loc = locs[slot]
    base = source[slot]
    rows = []
    for a in range(2):
        for b in range(2):
            w = loc[2 * di + a : 2 * di + a + 1] * loc[8 + 2 * dj + b : 9 + 2 * dj + b]
            rows.append(w * base)
    high, low = split_bf16(jnp.concatenate(rows, axis=0))
    both = pair[slot]
    return lax.dot_general(
        jnp.concatenate([high, low], axis=1),
        jnp.concatenate([both, both], axis=1),
        (((1,), (1,)), ((), ())),
        preferred_element_type=jnp.float32,
    )


def own_gram_kernel(slab0_ref, slab1_ref, ens_ref, gram_ref, stack_ref, mean_ref, source, pair, locs):
    def put(c, carry):
        for i, ref in enumerate((slab0_ref, slab1_ref)):
            put_slab(i * EXT_COLS + c, ref, c * SLAB, source, pair, locs)
        return carry

    lax.fori_loop(0, EXT_COLS, put, 0)

    def one(c, carry):
        for i in range(ROWS):
            acc = jnp.zeros((POINTS * MEMBERS, 2 * WIDE), jnp.float32)
            for q in range(ROWS):
                for dj in range(3):
                    acc = acc + contribution(q * EXT_COLS + c + dj, q - i + 1, dj, source, pair, locs)
            for p in range(POINTS):
                gram_ref[pl.ds((i * COLS + c) * BLOCK_MAT + p * MAT, MEMBERS), 0 : 2 * WIDE] = acc[
                    p * MEMBERS : (p + 1) * MEMBERS
                ]
        return carry

    lax.fori_loop(0, COLS, one, 0, unroll=4)

    def stack(c, carry):
        for i in range(ROWS):
            block = i * COLS + c
            for t in range(4):
                ens = ens_ref[pl.ds(first_row(i, c) + 8 * t, MEMBERS, stride=PITCH), :]
                mean = jnp.sum(ens, axis=0, keepdims=True) * (1.0 / MEMBERS)
                mean_ref[pl.ds(block * 4 + t, 1), :] = mean
                anomaly = ens - mean
                high = anomaly.astype(jnp.bfloat16).astype(jnp.float32)
                rows = jnp.concatenate(
                    [high, anomaly - high, high, jnp.zeros((STACK - 3 * MEMBERS, 128), jnp.float32)], axis=0
                )
                f, a = t // 2, t % 2
                stack_ref[2 * block + a, :, 128 * f : 128 * f + 128] = rows.astype(jnp.bfloat16)
        return carry

    lax.fori_loop(0, COLS, stack, 0, unroll=2)


def sym_product(left, right, out, finish):
    for tile in range(3):
        lo = 8 * tile
        for half in range(2):
            i0 = lo + 4 * half
            acc = [None] * 4
            for k in range(MEMBERS):
                row = right[k * MAT + lo : k * MAT + MEMBERS, :]
                for step in range(4):
                    at = (i0 + step) * MAT + k
                    term = left[at : at + 1, :] * row
                    acc[step] = term if acc[step] is None else acc[step] + term
            for step in range(4):
                i = i0 + step
                row = finish(acc[step], i, lo)
                out[i * MAT + lo : i * MAT + MEMBERS, :] = row
                for j in range(tile + 1, 3):
                    out[pl.ds(8 * j * MAT + i, 8, stride=MAT), :] = row[8 * (j - tile) : 8 * (j - tile) + 8]


def plain(row, i, lo):
    return row


def newton_step(row, i, lo):
    where = lax.broadcasted_iota(jnp.int32, row.shape, 0) + lo
    return jnp.where(where == i, 1.5, 0.0) - 0.5 * row


def analyze_kernel(m_ref, stack_ref, mean_ref, own_ref, above_ref, below_ref, *refs):
    outs = refs[:GROUPS]
    source, pair, locs, gram, ya, yb, za, zb, mm, drive, moved_ref = refs[GROUPS:]
    m = m_ref[0]

    def put(c, carry):
        put_slab(c, above_ref, c * SLAB, source, pair, locs)
        put_slab(EXT_COLS + c, below_ref, c * SLAB, source, pair, locs)
        return carry

    lax.fori_loop(0, EXT_COLS, put, 0)

    def one_gram(c, carry):
        for i in range(ROWS):
            acc = jnp.zeros((POINTS * MEMBERS, 2 * WIDE), jnp.float32)
            for dj in range(3):
                acc = acc + contribution(i * EXT_COLS + c + dj, 2 * i, dj, source, pair, locs)
            for p in range(POINTS):
                at = (i * COLS + c) * BLOCK_MAT + p * MAT
                gram[pl.ds(at, MEMBERS), 0 : 2 * WIDE] = (
                    own_ref[pl.ds(at, MEMBERS), 0 : 2 * WIDE] + acc[p * MEMBERS : (p + 1) * MEMBERS]
                )
        return carry

    lax.fori_loop(0, COLS, one_gram, 0, unroll=8)
    member = lax.broadcasted_iota(jnp.int32, (MEMBERS, 128), 0)
    squares = jnp.zeros((MEMBERS, 128), jnp.float32)
    for k in range(MEMBERS):
        turned = gram[pl.ds(k, 128, stride=MAT), :].T
        total = turned[0:WIDE] + turned[WIDE : 2 * WIDE]
        row = total[0:MEMBERS] + jnp.where(member == k, (MEMBERS - 1) / INFLATION_FACTOR, 0.0)
        drive[k : k + 1, :] = total[MEMBERS : MEMBERS + 1]
        ya[k * MAT : k * MAT + MEMBERS, :] = row
        squares = squares + row * row
    norm = jnp.sqrt(jnp.sum(squares, axis=0, keepdims=True))
    inverse = 1.0 / norm
    for k in range(MEMBERS):
        row = ya[k * MAT : k * MAT + MEMBERS, :] * inverse
        ya[k * MAT : k * MAT + MEMBERS, :] = row
        za[k * MAT : k * MAT + MEMBERS, :] = newton_step(row, k, 0)

    sym_product(ya, za, yb, plain)

    def two_steps(turn, carry):
        sym_product(za, yb, mm, newton_step)
        sym_product(yb, mm, ya, plain)
        sym_product(mm, za, zb, plain)
        sym_product(zb, ya, mm, newton_step)
        sym_product(ya, mm, yb, plain)
        sym_product(mm, zb, za, plain)
        return carry

    lax.fori_loop(0, (NS_ITERS - 2) // 2, two_steps, 0)
    sym_product(za, yb, mm, newton_step)
    sym_product(mm, za, zb, plain)

    scale = 1.0 / jnp.sqrt(norm)
    half_way = jnp.zeros((MEMBERS, 128), jnp.float32)
    for k in range(MEMBERS):
        half_way = half_way + zb[k * MAT : k * MAT + MEMBERS, :] * drive[k : k + 1, :]
    half_way = half_way * scale
    mean_w = jnp.zeros((MEMBERS, 128), jnp.float32)
    for k in range(MEMBERS):
        mean_w = mean_w + zb[k * MAT : k * MAT + MEMBERS, :] * half_way[k : k + 1]
    mean_w = mean_w * scale
    spread = scale * math.sqrt(MEMBERS - 1)
    blank = jnp.zeros((128 - 3 * MEMBERS, 128), jnp.float32)
    for k in range(MEMBERS):
        weight = mean_w + spread * zb[k * MAT : k * MAT + MEMBERS, :]
        high = weight.astype(jnp.bfloat16).astype(jnp.float32)
        gram[pl.ds(k, 128, stride=MAT), :] = jnp.concatenate(
            [high, high, weight - high, blank], axis=0
        ).T

    right_half = (lax.broadcasted_iota(jnp.int32, (MEMBERS, 128), 1) >> 3) & 1

    def one_update(c, carry):
        for i in range(ROWS):
            at = (i * COLS + c) * BLOCK_MAT
            first = first_row(i, c)
            for a in range(2):
                values = jnp.concatenate(
                    [stack_ref[2 * (i * COLS + c) + a], jnp.zeros((128 - STACK, 256), jnp.bfloat16)], axis=0
                )
                weight = jnp.concatenate(
                    [gram[pl.ds(at + (2 * a + b) * MAT, MEMBERS), :] for b in range(2)], axis=0
                ).astype(jnp.bfloat16)
                moved = jnp.dot(weight, values, preferred_element_type=jnp.float32)
                for f in range(2):
                    part = moved[:, 128 * f : 128 * f + 128]
                    t = 2 * f + a
                    moved_tile = jnp.where(right_half == 1, part[MEMBERS:], part[:MEMBERS])
                    moved_ref[pl.ds(first + 8 * t, MEMBERS, stride=PITCH), :] = (
                        mean_ref[pl.ds((i * COLS + c) * 4 + t, 1), :] + moved_tile
                    )
        return carry

    lax.fori_loop(0, COLS, one_update, 0, unroll=8)
    for s in range(GROUPS):
        for k in range(HELD):
            start = ((m ^ s) * HELD + k) * PITCH
            outs[s][k * FIELD_ROWS : (k + 1) * FIELD_ROWS, :] = moved_ref[pl.ds(start, FIELD_ROWS), :]


def f32(*shape):
    return jax.ShapeDtypeStruct(shape, jnp.float32)


def tables(slots):
    return [
        pltpu.VMEM((slots, MEMBERS, OBS), jnp.float32),
        pltpu.VMEM((slots, 2 * WIDE, OBS), jnp.bfloat16),
        pltpu.VMEM((slots, 16, OBS), jnp.float32),
    ]


def vmem_call(kernel, out_shape, flops, args, scratch=()):
    places = [
        pl.BlockSpec(memory_space=pltpu.SMEM if x.dtype == jnp.int32 else pltpu.VMEM) for x in args
    ]
    return pl.pallas_call(
        kernel,
        out_shape=out_shape,
        in_specs=places,
        scratch_shapes=list(scratch),
        cost_estimate=pl.CostEstimate(flops=flops, bytes_accessed=0, transcendentals=0),
        compiler_params=pltpu.CompilerParams(vmem_limit_bytes=32 * 1024 * 1024),
    )(*args)


def swapped(x, s):
    return lax.ppermute(x, "member", [(a, a ^ s) for a in range(GROUPS)])


def paired(x, start):
    regions = lax.axis_size("region")
    pairs = []
    for a in range(start, regions - 1, 2):
        pairs += [(a, a + 1), (a + 1, a)]
    return lax.ppermute(x, "region", pairs)


def edge_columns(x):
    members, regions = lax.axis_size("member"), lax.axis_size("region")
    pairs = []
    for a in range(members - 1):
        pairs.append((a * regions + regions - 1, (a + 1) * regions + regions - 1))
        pairs.append(((a + 1) * regions, a * regions))
    return lax.ppermute(x, ("member", "region"), pairs)


def local(ensemble, obs_value, obs_error, obs_index, obs_count):
    m = lax.axis_index("member").astype(jnp.int32)
    where = m.reshape(1)
    tiled = ensemble.reshape(HELD, ROWS, 2 * GROUPS, 8, 4, 128).transpose(0, 1, 2, 4, 3, 5).reshape(-1, 128)
    pieces = pl.pallas_call(
        pack_kernel,
        out_shape=[f32(PART_ROWS, 128)] * GROUPS,
        in_specs=[pl.BlockSpec(memory_space=pltpu.SMEM), pl.BlockSpec(memory_space=pltpu.HBM)],
        scratch_shapes=[
            pltpu.VMEM((HELD * ROWS * GROUPS * 64, 128), jnp.float32),
            pltpu.SemaphoreType.DMA((HELD * ROWS,)),
        ],
        compiler_params=pltpu.CompilerParams(vmem_limit_bytes=54000000),
    )(where, tiled)
    slot = lax.broadcasted_iota(jnp.int32, (32, 1, OBS), 2)
    live = jnp.where(slot < obs_count[:, :, None], 1.0, 0.0).astype(jnp.float32)
    root_weight = jnp.sqrt(live / obs_error)
    columns = [obs_value, root_weight, obs_index.astype(jnp.float32), jnp.zeros_like(obs_value)]
    packed = jnp.concatenate([x.reshape(COLS, ROWS, OBS) for x in columns], axis=1)
    beside = edge_columns(packed)
    packed = jnp.concatenate([packed, beside], axis=1)
    parts = [swapped(pieces[s], s) if s else pieces[s] for s in range(GROUPS)]

    obs = lax.all_to_all(packed, "region", split_axis=0, concat_axis=0, tiled=True)

    ens, slab0, slab1 = vmem_call(
        observe_kernel,
        (f32(MEMBERS * PITCH, 128), f32(SLAB_ROWS, OBS), f32(SLAB_ROWS, OBS)),
        10**9,
        [where, *parts, obs],
        [pltpu.VMEM((MEMBERS * EDGE_PITCH, 128), jnp.float32)],
    )

    odd = (lax.axis_index("region") & 1) == 1
    first = paired(jnp.where(odd, slab0, slab1), 0)
    second = paired(jnp.where(odd, slab1, slab0), 1)
    above = jnp.where(odd, first, second)
    below = jnp.where(odd, second, first)

    own, stack, mean = vmem_call(
        own_gram_kernel,
        (
            f32(BLOCKS * BLOCK_MAT, 128),
            jax.ShapeDtypeStruct((2 * BLOCKS, STACK, 256), jnp.bfloat16),
            f32(BLOCKS * 4, 128),
        ),
        4 * 10**9,
        [slab0, slab1, ens],
        tables(ROWS * EXT_COLS),
    )

    square = pltpu.VMEM((MEMBERS * MAT, 128), jnp.float32)
    moved = vmem_call(
        analyze_kernel,
        [f32(HELD * FIELD_ROWS, 128)] * GROUPS,
        10**10,
        [where, stack, mean, own, above, below],
        tables(ROWS * EXT_COLS)
        + [
            pltpu.VMEM((BLOCKS * BLOCK_MAT, 128), jnp.float32),
            square, square, square, square, square,
            pltpu.VMEM((MEMBERS, 128), jnp.float32),
            pltpu.VMEM((MEMBERS * PITCH, 128), jnp.float32),
        ],
    )

    result = jnp.zeros((HELD, ROWS, GROUPS, 2, 4, 8, 128), jnp.float32)
    for s in range(GROUPS):
        part = swapped(moved[s], s) if s else moved[s]
        part = part.reshape(HELD, ROWS, 1, 2, 4, 8, 128)
        result = lax.dynamic_update_slice_in_dim(result, part, m ^ s, 2)
    return result.transpose(0, 1, 2, 3, 5, 4, 6).reshape(HELD, ROWS, GROUPS * COLS, VALS)


def solution(mesh):
    return jax.shard_map(
        local,
        mesh=mesh,
        in_specs=(
            P("member", "region", None, None),
            P(None, ("member", "region"), None),
            P(None, ("member", "region"), None),
            P(None, ("member", "region"), None),
            P(None, ("member", "region")),
        ),
        out_specs=P("member", "region", None, None),
        check_vma=False,
    )
```

```python
import math

import jax
import jax.numpy as jnp
from jax import lax
from jax.experimental import pallas as pl
from jax.experimental.pallas import tpu as pltpu
from jax.sharding import PartitionSpec as P


SIDE = 16
NS_ITERS = 6
MEMBERS = 24
OBS = 128
VALS = 512
INFLATION_FACTOR = 1.1
INV_SCALE = 1.0 / 288.0

GROUPS = 8
HELD = MEMBERS // GROUPS
ROWS = 2
COLS = 16
BLOCKS = ROWS * COLS
POINTS = 4
EXT_COLS = COLS + 2
FIELD_ROWS = BLOCKS * 4
PITCH = FIELD_ROWS + 4
SLAB = 26
WIDE = 32
STACK = 80
SLAB_ROWS = 472
EDGE_PITCH = 20
PART_ROWS = HELD * (FIELD_ROWS + 16)
MAT = MEMBERS + 4
BLOCK_MAT = POINTS * MAT


def first_row(i, c):
    return i * 64 + (c >> 3) * 32 + (c & 7)


def split_bf16(x):
    high = x.astype(jnp.bfloat16)
    low = (x - high.astype(jnp.float32)).astype(jnp.bfloat16)
    return high, low


def pack_kernel(m_ref, ens_ref, *refs):
    outs = refs[:GROUPS]
    stage, sems = refs[GROUPS:]
    m = m_ref[0]
    tiles = GROUPS * 8
    chunk_rows = tiles * 8
    copies = []
    for n in range(HELD * ROWS):
        copy = pltpu.make_async_copy(
            ens_ref.at[pl.ds(n * chunk_rows, chunk_rows), :],
            stage.at[pl.ds(n * chunk_rows, chunk_rows), :],
            sems.at[n],
        )
        copy.start()
        copies.append(copy)

    for n in range(HELD * ROWS):
        k, i = n // ROWS, n % ROWS
        copies[n].wait()
        for s in range(GROUPS):
            to = m ^ s
            start = pl.multiple_of(n * chunk_rows + to * 64, 64)
            outs[s][n * 64 : n * 64 + 64, :] = stage[pl.ds(start, 64), :]
            before = jnp.maximum(2 * to - 1, 0) * 32 + 7
            after = jnp.minimum(2 * to + 2, 2 * GROUPS - 1) * 32
            for e, at in enumerate((before, after)):
                row = HELD * FIELD_ROWS + (e * HELD + k) * 8 + 4 * i
                outs[s][row : row + 4, :] = stage[pl.ds(n * chunk_rows + at, 4, stride=8), :]


def observe_kernel(m_ref, *refs):
    parts = refs[:GROUPS]
    obs_ref, ens_ref, slab0_ref, slab1_ref, edge = refs[GROUPS:]
    slabs = (slab0_ref, slab1_ref)
    m = m_ref[0]
    for s in range(GROUPS):
        for k in range(HELD):
            member = (m ^ s) * HELD + k
            ens_ref[pl.ds(member * PITCH, FIELD_ROWS), :] = parts[s][
                k * FIELD_ROWS : (k + 1) * FIELD_ROWS, :
            ]
            for e in range(2):
                at = HELD * FIELD_ROWS + (e * HELD + k) * 8
                edge[pl.ds(member * EDGE_PITCH + 8 * e, 8), :] = parts[s][at : at + 8, :]

    def one(i, slot, obs, load):
        value = obs[i : i + 1]
        weight = obs[2 + i : 3 + i]
        index_f = obs[4 + i : 5 + i]
        index = jnp.broadcast_to(index_f.astype(jnp.int32), (MEMBERS, OBS))
        lane = index & 127
        chunk = index >> 7
        seen = jnp.zeros((MEMBERS, OBS), jnp.float32)
        for t in range(4):
            got = jnp.take_along_axis(load(t), lane, axis=1, mode="promise_in_bounds")
            seen = jnp.where(chunk == t, got, seen)
        mean = jnp.sum(seen, axis=0, keepdims=True) * (1.0 / MEMBERS)
        base = slot * SLAB
        slabs[i][pl.ds(base, MEMBERS), :] = weight * (seen - mean)
        slabs[i][pl.ds(base + MEMBERS, 1), :] = weight * (value - mean)
        slabs[i][pl.ds(base + MEMBERS + 1, 1), :] = index_f

    def body(c, carry):
        obs = obs_ref[c]
        for i in range(ROWS):
            one(i, c + 1, obs, lambda t: ens_ref[pl.ds(first_row(i, c) + 8 * t, MEMBERS, stride=PITCH), :])
        return carry

    lax.fori_loop(0, COLS, body, 0, unroll=16)
    for e, source in enumerate((COLS - 1, 0)):
        obs = obs_ref[source, 8:16, :]
        for i in range(ROWS):
            one(
                i,
                e * (EXT_COLS - 1),
                obs,
                lambda t: edge[pl.ds(8 * e + 4 * i + t, MEMBERS, stride=EDGE_PITCH), :],
            )


def put_slab(slot, ref, base, source, pair, locs):
    t = lax.broadcasted_iota(jnp.int32, (8, OBS), 0)
    offset = (((t >> 1) - 1) * SIDE - (t & 1) * 8).astype(jnp.float32) - 3.5
    cell = ref[pl.ds(base + MEMBERS + 1, 1), :].astype(jnp.int32) & 255
    dy = (cell >> 4).astype(jnp.float32) + offset
    dx = (cell & 15).astype(jnp.float32) + offset
    locs[slot, 0:8, :] = jnp.exp(-(dy * dy) * INV_SCALE)
    locs[slot, 8:16, :] = jnp.exp(-(dx * dx) * INV_SCALE)
    scaled = ref[pl.ds(base, MEMBERS), :]
    source[slot] = scaled
    innovation = jnp.broadcast_to(ref[pl.ds(base + MEMBERS, 1), :], (8, OBS))
    high, low = split_bf16(jnp.concatenate([scaled, innovation], axis=0))
    pair[slot] = jnp.concatenate([high, low], axis=0)


def contribution(slot, di, dj, source, pair, locs):
    loc = locs[slot]
    base = source[slot]
    rows = []
    for a in range(2):
        for b in range(2):
            w = loc[2 * di + a : 2 * di + a + 1] * loc[8 + 2 * dj + b : 9 + 2 * dj + b]
            rows.append(w * base)
    high, low = split_bf16(jnp.concatenate(rows, axis=0))
    both = pair[slot]
    return lax.dot_general(
        jnp.concatenate([high, low], axis=1),
        jnp.concatenate([both, both], axis=1),
        (((1,), (1,)), ((), ())),
        preferred_element_type=jnp.float32,
    )


def own_gram_kernel(slab0_ref, slab1_ref, ens_ref, gram_ref, stack_ref, mean_ref, source, pair, locs):
    def put(c, carry):
        for i, ref in enumerate((slab0_ref, slab1_ref)):
            put_slab(i * EXT_COLS + c, ref, c * SLAB, source, pair, locs)
        return carry

    lax.fori_loop(0, EXT_COLS, put, 0, unroll=6)

    def one(c, carry):
        for i in range(ROWS):
            acc = jnp.zeros((POINTS * MEMBERS, 2 * WIDE), jnp.float32)
            for q in range(ROWS):
                for dj in range(3):
                    acc = acc + contribution(q * EXT_COLS + c + dj, q - i + 1, dj, source, pair, locs)
            for p in range(POINTS):
                gram_ref[pl.ds((i * COLS + c) * BLOCK_MAT + p * MAT, MEMBERS), 0 : 2 * WIDE] = acc[
                    p * MEMBERS : (p + 1) * MEMBERS
                ]
        return carry

    lax.fori_loop(0, COLS, one, 0, unroll=4)

    def stack(c, carry):
        for i in range(ROWS):
            block = i * COLS + c
            for t in range(4):
                ens = ens_ref[pl.ds(first_row(i, c) + 8 * t, MEMBERS, stride=PITCH), :]
                mean = jnp.sum(ens, axis=0, keepdims=True) * (1.0 / MEMBERS)
                mean_ref[pl.ds(block * 4 + t, 1), :] = mean
                anomaly = ens - mean
                high = anomaly.astype(jnp.bfloat16).astype(jnp.float32)
                rows = jnp.concatenate(
                    [high, anomaly - high, high, jnp.zeros((STACK - 3 * MEMBERS, 128), jnp.float32)], axis=0
                )
                f, a = t // 2, t % 2
                stack_ref[2 * block + a, :, 128 * f : 128 * f + 128] = rows.astype(jnp.bfloat16)
        return carry

    lax.fori_loop(0, COLS, stack, 0, unroll=2)


def sym_product(left, right, out, finish):
    for tile in range(3):
        lo = 8 * tile
        for half in range(2):
            i0 = lo + 4 * half
            acc = [None] * 4
            for k in range(MEMBERS):
                row = right[k * MAT + lo : k * MAT + MEMBERS, :]
                for step in range(4):
                    at = (i0 + step) * MAT + k
                    term = left[at : at + 1, :] * row
                    acc[step] = term if acc[step] is None else acc[step] + term
            for step in range(4):
                i = i0 + step
                row = finish(acc[step], i, lo)
                out[i * MAT + lo : i * MAT + MEMBERS, :] = row
                for j in range(tile + 1, 3):
                    out[pl.ds(8 * j * MAT + i, 8, stride=MAT), :] = row[8 * (j - tile) : 8 * (j - tile) + 8]


def plain(row, i, lo):
    return row


def newton_step(row, i, lo):
    where = lax.broadcasted_iota(jnp.int32, row.shape, 0) + lo
    return jnp.where(where == i, 1.5, 0.0) - 0.5 * row


def analyze_kernel(m_ref, stack_ref, mean_ref, own_ref, above_ref, below_ref, *refs):
    outs = refs[:GROUPS]
    source, pair, locs, gram, ya, yb, za, zb, mm, drive, moved_ref = refs[GROUPS:]
    m = m_ref[0]

    def put(c, carry):
        put_slab(c, above_ref, c * SLAB, source, pair, locs)
        put_slab(EXT_COLS + c, below_ref, c * SLAB, source, pair, locs)
        return carry

    lax.fori_loop(0, EXT_COLS, put, 0, unroll=6)

    def one_gram(c, carry):
        for i in range(ROWS):
            acc = jnp.zeros((POINTS * MEMBERS, 2 * WIDE), jnp.float32)
            for dj in range(3):
                acc = acc + contribution(i * EXT_COLS + c + dj, 2 * i, dj, source, pair, locs)
            for p in range(POINTS):
                at = (i * COLS + c) * BLOCK_MAT + p * MAT
                gram[pl.ds(at, MEMBERS), 0 : 2 * WIDE] = (
                    own_ref[pl.ds(at, MEMBERS), 0 : 2 * WIDE] + acc[p * MEMBERS : (p + 1) * MEMBERS]
                )
        return carry

    lax.fori_loop(0, COLS, one_gram, 0, unroll=16)
    member = lax.broadcasted_iota(jnp.int32, (MEMBERS, 128), 0)
    squares = jnp.zeros((MEMBERS, 128), jnp.float32)
    for k in range(MEMBERS):
        turned = gram[pl.ds(k, 128, stride=MAT), :].T
        total = turned[0:WIDE] + turned[WIDE : 2 * WIDE]
        row = total[0:MEMBERS] + jnp.where(member == k, (MEMBERS - 1) / INFLATION_FACTOR, 0.0)
        drive[k : k + 1, :] = total[MEMBERS : MEMBERS + 1]
        ya[k * MAT : k * MAT + MEMBERS, :] = row
        squares = squares + row * row
    norm = jnp.sqrt(jnp.sum(squares, axis=0, keepdims=True))
    inverse = 1.0 / norm
    for k in range(MEMBERS):
        row = ya[k * MAT : k * MAT + MEMBERS, :] * inverse
        ya[k * MAT : k * MAT + MEMBERS, :] = row
        za[k * MAT : k * MAT + MEMBERS, :] = newton_step(row, k, 0)

    sym_product(ya, za, yb, plain)

    def two_steps(turn, carry):
        sym_product(za, yb, mm, newton_step)
        sym_product(yb, mm, ya, plain)
        sym_product(mm, za, zb, plain)
        sym_product(zb, ya, mm, newton_step)
        sym_product(ya, mm, yb, plain)
        sym_product(mm, zb, za, plain)
        return carry

    lax.fori_loop(0, (NS_ITERS - 2) // 2, two_steps, 0)
    sym_product(za, yb, mm, newton_step)
    sym_product(mm, za, zb, plain)

    scale = 1.0 / jnp.sqrt(norm)
    half_way = jnp.zeros((MEMBERS, 128), jnp.float32)
    for k in range(MEMBERS):
        half_way = half_way + zb[k * MAT : k * MAT + MEMBERS, :] * drive[k : k + 1, :]
    half_way = half_way * scale
    mean_w = jnp.zeros((MEMBERS, 128), jnp.float32)
    for k in range(MEMBERS):
        mean_w = mean_w + zb[k * MAT : k * MAT + MEMBERS, :] * half_way[k : k + 1]
    mean_w = mean_w * scale
    spread = scale * math.sqrt(MEMBERS - 1)
    blank = jnp.zeros((128 - 3 * MEMBERS, 128), jnp.float32)
    for k in range(MEMBERS):
        weight = mean_w + spread * zb[k * MAT : k * MAT + MEMBERS, :]
        high = weight.astype(jnp.bfloat16).astype(jnp.float32)
        gram[pl.ds(k, 128, stride=MAT), :] = jnp.concatenate(
            [high, high, weight - high, blank], axis=0
        ).T

    right_half = (lax.broadcasted_iota(jnp.int32, (MEMBERS, 128), 1) >> 3) & 1

    def one_update(c, carry):
        for i in range(ROWS):
            at = (i * COLS + c) * BLOCK_MAT
            first = first_row(i, c)
            for a in range(2):
                values = jnp.concatenate(
                    [stack_ref[2 * (i * COLS + c) + a], jnp.zeros((128 - STACK, 256), jnp.bfloat16)], axis=0
                )
                weight = jnp.concatenate(
                    [gram[pl.ds(at + (2 * a + b) * MAT, MEMBERS), :] for b in range(2)], axis=0
                ).astype(jnp.bfloat16)
                moved = jnp.dot(weight, values, preferred_element_type=jnp.float32)
                for f in range(2):
                    part = moved[:, 128 * f : 128 * f + 128]
                    t = 2 * f + a
                    moved_tile = jnp.where(right_half == 1, part[MEMBERS:], part[:MEMBERS])
                    moved_ref[pl.ds(first + 8 * t, MEMBERS, stride=PITCH), :] = (
                        mean_ref[pl.ds((i * COLS + c) * 4 + t, 1), :] + moved_tile
                    )
        return carry

    lax.fori_loop(0, COLS, one_update, 0, unroll=16)
    for s in range(GROUPS):
        for k in range(HELD):
            start = ((m ^ s) * HELD + k) * PITCH
            outs[s][k * FIELD_ROWS : (k + 1) * FIELD_ROWS, :] = moved_ref[pl.ds(start, FIELD_ROWS), :]


def f32(*shape):
    return jax.ShapeDtypeStruct(shape, jnp.float32)


def tables(slots):
    return [
        pltpu.VMEM((slots, MEMBERS, OBS), jnp.float32),
        pltpu.VMEM((slots, 2 * WIDE, OBS), jnp.bfloat16),
        pltpu.VMEM((slots, 16, OBS), jnp.float32),
    ]


def vmem_call(kernel, out_shape, flops, args, scratch=()):
    places = [
        pl.BlockSpec(memory_space=pltpu.SMEM if x.dtype == jnp.int32 else pltpu.VMEM) for x in args
    ]
    return pl.pallas_call(
        kernel,
        out_shape=out_shape,
        in_specs=places,
        scratch_shapes=list(scratch),
        cost_estimate=pl.CostEstimate(flops=flops, bytes_accessed=0, transcendentals=0),
        compiler_params=pltpu.CompilerParams(vmem_limit_bytes=32 * 1024 * 1024),
    )(*args)


def swapped(x, s):
    return lax.ppermute(x, "member", [(a, a ^ s) for a in range(GROUPS)])


def paired(x, start):
    regions = lax.axis_size("region")
    pairs = []
    for a in range(start, regions - 1, 2):
        pairs += [(a, a + 1), (a + 1, a)]
    return lax.ppermute(x, "region", pairs)


def edge_columns(x):
    members, regions = lax.axis_size("member"), lax.axis_size("region")
    pairs = []
    for a in range(members - 1):
        pairs.append((a * regions + regions - 1, (a + 1) * regions + regions - 1))
        pairs.append(((a + 1) * regions, a * regions))
    return lax.ppermute(x, ("member", "region"), pairs)


def local(ensemble, obs_value, obs_error, obs_index, obs_count):
    m = lax.axis_index("member").astype(jnp.int32)
    where = m.reshape(1)
    tiled = ensemble.reshape(HELD, ROWS, 2 * GROUPS, 8, 4, 128).transpose(0, 1, 2, 4, 3, 5).reshape(-1, 128)
    pieces = pl.pallas_call(
        pack_kernel,
        out_shape=[f32(PART_ROWS, 128)] * GROUPS,
        in_specs=[pl.BlockSpec(memory_space=pltpu.SMEM), pl.BlockSpec(memory_space=pltpu.HBM)],
        scratch_shapes=[
            pltpu.VMEM((HELD * ROWS * GROUPS * 64, 128), jnp.float32),
            pltpu.SemaphoreType.DMA((HELD * ROWS,)),
        ],
        compiler_params=pltpu.CompilerParams(vmem_limit_bytes=54000000),
    )(where, tiled)
    slot = lax.broadcasted_iota(jnp.int32, (32, 1, OBS), 2)
    live = jnp.where(slot < obs_count[:, :, None], 1.0, 0.0).astype(jnp.float32)
    root_weight = jnp.sqrt(live / obs_error)
    columns = [obs_value, root_weight, obs_index.astype(jnp.float32), jnp.zeros_like(obs_value)]
    packed = jnp.concatenate([x.reshape(COLS, ROWS, OBS) for x in columns], axis=1)
    beside = edge_columns(packed)
    packed = jnp.concatenate([packed, beside], axis=1)
    parts = [swapped(pieces[s], s) if s else pieces[s] for s in range(GROUPS)]

    obs = lax.all_to_all(packed, "region", split_axis=0, concat_axis=0, tiled=True)

    ens, slab0, slab1 = vmem_call(
        observe_kernel,
        (f32(MEMBERS * PITCH, 128), f32(SLAB_ROWS, OBS), f32(SLAB_ROWS, OBS)),
        10**9,
        [where, *parts, obs],
        [pltpu.VMEM((MEMBERS * EDGE_PITCH, 128), jnp.float32)],
    )

    odd = (lax.axis_index("region") & 1) == 1
    first = paired(jnp.where(odd, slab0, slab1), 0)
    second = paired(jnp.where(odd, slab1, slab0), 1)
    above = jnp.where(odd, first, second)
    below = jnp.where(odd, second, first)

    own, stack, mean = vmem_call(
        own_gram_kernel,
        (
            f32(BLOCKS * BLOCK_MAT, 128),
            jax.ShapeDtypeStruct((2 * BLOCKS, STACK, 256), jnp.bfloat16),
            f32(BLOCKS * 4, 128),
        ),
        4 * 10**9,
        [slab0, slab1, ens],
        tables(ROWS * EXT_COLS),
    )

    square = pltpu.VMEM((MEMBERS * MAT, 128), jnp.float32)
    moved = vmem_call(
        analyze_kernel,
        [f32(HELD * FIELD_ROWS, 128)] * GROUPS,
        10**10,
        [where, stack, mean, own, above, below],
        tables(ROWS * EXT_COLS)
        + [
            pltpu.VMEM((BLOCKS * BLOCK_MAT, 128), jnp.float32),
            square, square, square, square, square,
            pltpu.VMEM((MEMBERS, 128), jnp.float32),
            pltpu.VMEM((MEMBERS * PITCH, 128), jnp.float32),
        ],
    )

    result = jnp.zeros((HELD, ROWS, GROUPS, 2, 4, 8, 128), jnp.float32)
    for s in range(GROUPS):
        part = swapped(moved[s], s) if s else moved[s]
        part = part.reshape(HELD, ROWS, 1, 2, 4, 8, 128)
        result = lax.dynamic_update_slice_in_dim(result, part, m ^ s, 2)
    return result.transpose(0, 1, 2, 3, 5, 4, 6).reshape(HELD, ROWS, GROUPS * COLS, VALS)


def solution(mesh):
    return jax.shard_map(
        local,
        mesh=mesh,
        in_specs=(
            P("member", "region", None, None),
            P(None, ("member", "region"), None),
            P(None, ("member", "region"), None),
            P(None, ("member", "region"), None),
            P(None, ("member", "region")),
        ),
        out_specs=P("member", "region", None, None),
        check_vma=False,
    )
```
